256 devices in a mesh: groups: 2 (over y), nodes: 128 (over z, x, core).
Axes of the slice: x: 4, y: 2, z: 16, core: 2. Of those that a mesh axis runs over, the one named last changes fastest.
The devices are a block of a 4x16x16 slice.
Arguments:
- grid_latents: bfloat16 [262144, 1024], P(('groups', 'nodes')), parts along dimension 0, may hold values from -16 to 16
- mesh_latents: bfloat16 [65536, 1024], P(('groups', 'nodes')), parts along dimension 0, may hold values from -16 to 16
- neighbour_tiles: int32 [256, 6], P('nodes'), may hold values from 0 to 1023, as said below
- neighbour_live: int32 [256, 6], P('nodes'), may hold values from 0 to 1, as said below
- w_query: bfloat16 [1024, 1024], replicated, may hold values from -0.1875 to 0.1875
- w_keyval: bfloat16 [1024, 2048], replicated, may hold values from -0.1875 to 0.1875
- w_out: bfloat16 [1024, 1024], replicated, may hold values from -0.375 to 0.375
Outputs:
- mesh_next: float32 [65536, 1024], P(('groups', 'nodes')), parts along dimension 0
The draws below stay inside these ranges and needn't reach their ends.
There are 2 independent parts, one for each index of `groups`. The reference program is written for one: setup_inputs(seed, part) draws one part's arguments, and reference() takes and returns one part's arrays. A program takes and returns all parts, laid end to end along the dimension named above; an argument that names none is the same for every part. Nothing has to cross between parts.
Inputs may be any that keep to these rules, and one draw needn't show every extreme that they name: `neighbour_tiles`: tile t lies on device t // 8 along nodes and mesh tile m on device m // 2; every listed tile lies on a device at most 2 indices away cyclically. The 6 entries of one mesh tile are distinct. Among the live entries of one device's mesh tiles at most 2 distinct tiles come from any one other device, and on every device some other device gives exactly 2. `neighbour_live`: each mesh tile has 2 to 6 live entries.
All inputs are finite; a program needn't handle non-finite values.
Results may differ from the reference program's by a relative error of at most 0.002.
The reference program's roundings to bfloat16 on the way count: a program that leaves them out, or rounds other values in their place, can miss the bound.
Values may be sent and summed in bfloat16 or wider, within the bound.
No kernel may reach another device: no remote copies, remote signals or barrier semaphores. Data moves between devices by JAX's collectives and lax.ppermute only.
A program may use at most 128 MiB of HBM per device.

```python
import jax
import jax.numpy as jnp
from jax import lax

C = 1024
HEADS = 16
TILE = 128
NB = 6
REACH = 2
CAP = 2
GT_DEV = 8
MT_DEV = 2
GRID = 131072
MESH = 32768
N_NODES = 128


def neighbour_plan(key):
    base = jax.random.fold_in(key, 7)
    key_sets, key_order, key_count, key_rank = jax.random.split(base, 4)
    node_total = N_NODES
    offset_count = 2 * REACH
    candidates = GT_DEV + offset_count * CAP
    spread = jnp.arange(GT_DEV, dtype=jnp.int32)
    set_scores = jax.random.randint(key_sets, (node_total, offset_count, GT_DEV), 0, 1 << 20) * GT_DEV + spread
    picked = jnp.argsort(set_scores, axis=-1)[:, :, :CAP].astype(jnp.int32)
    offsets = jnp.concatenate([jnp.arange(-REACH, 0), jnp.arange(1, REACH + 1)]).astype(jnp.int32)
    devices = jnp.arange(node_total, dtype=jnp.int32)
    sources = (devices[:, None] + offsets[None, :] + node_total) % node_total
    remote = sources[:, :, None] * GT_DEV + picked
    owned = devices[:, None] * GT_DEV + spread[None, :]
    pooled = jnp.concatenate([owned, remote.reshape(node_total, offset_count * CAP)], axis=1)
    columns = jnp.arange(candidates, dtype=jnp.int32)
    order_scores = jax.random.randint(key_order, (node_total, MT_DEV, candidates), 0, 1 << 20) * candidates + columns
    forced_low = GT_DEV + devices % offset_count * CAP
    forced = (columns[None, :] >= forced_low[:, None]) & (columns[None, :] < forced_low[:, None] + CAP)
    first_tile = (jnp.arange(MT_DEV) == 0)[None, :, None]
    order_scores = jnp.where(forced[:, None, :] & first_tile, (columns - candidates)[None, None, :], order_scores)
    ordering = jnp.argsort(order_scores, axis=-1)[:, :, :NB]
    spread_pool = jnp.broadcast_to(pooled[:, None, :], (node_total, MT_DEV, candidates))
    tiles = jnp.take_along_axis(spread_pool, ordering, axis=-1)
    live_count = jax.random.randint(key_count, (node_total, MT_DEV), 2, NB + 1)
    live_count = jnp.where(jnp.arange(MT_DEV)[None, :] == 0, jnp.maximum(live_count, CAP), live_count)
    slot_ids = jnp.arange(NB, dtype=jnp.int32)
    rank_scores = jax.random.randint(key_rank, (node_total, MT_DEV, NB), 0, 1 << 20) * NB + slot_ids
    first_slots = first_tile & (slot_ids < CAP)[None, None, :]
    rank_scores = jnp.where(first_slots, (slot_ids - NB)[None, None, :], rank_scores)
    ranks = jnp.argsort(jnp.argsort(rank_scores, axis=-1), axis=-1)
    live = (ranks < live_count[:, :, None]).astype(jnp.int32)
    return (tiles.reshape(node_total * MT_DEV, NB).astype(jnp.int32), live.reshape(node_total * MT_DEV, NB))


def draw_neighbour_tiles(key, part):
    return neighbour_plan(key)[0]


def draw_neighbour_live(key, part):
    return neighbour_plan(key)[1]


def draw_grid_latents(key, part):
    key_values = jax.random.fold_in(jax.random.fold_in(key, 11), 0)
    values = jnp.clip(jax.random.normal(key_values, (GRID, C)), -6.0, 6.0)
    return values.astype(jnp.float32).astype(jnp.bfloat16)


def draw_mesh_latents(key, part):
    key_values = jax.random.fold_in(jax.random.fold_in(key, 13), 0)
    values = jnp.clip(2.0 * jax.random.normal(key_values, (MESH, C)), -12.0, 12.0)
    return values.astype(jnp.float32).astype(jnp.bfloat16)


def scatter_about(key, dims, scale, bound, held_as=jnp.bfloat16):
    return jnp.clip(scale * jax.random.normal(key, dims, jnp.float32), -bound, bound).astype(held_as)


def setup_inputs(seed: int = 0, part: int = 0) -> dict:
    streams_of = jax.random.split(jax.random.key(seed), 8)
    own_keys = jax.random.split(jax.random.fold_in(streams_of[7], part), 8)
    grid_latents = draw_grid_latents(jax.random.fold_in(jax.random.fold_in(streams_of[7], part), 71), part)
    mesh_latents = draw_mesh_latents(jax.random.fold_in(jax.random.fold_in(streams_of[7], part), 71), part)
    neighbour_tiles = draw_neighbour_tiles(jax.random.fold_in(streams_of[7], 71), part)
    neighbour_live = draw_neighbour_live(jax.random.fold_in(streams_of[7], 71), part)
    w_query = scatter_about(streams_of[4], (C, C), C ** -0.5, 0.1875)
    w_keyval = scatter_about(streams_of[5], (C, 2 * C), C ** -0.5, 0.1875)
    w_out = scatter_about(streams_of[6], (C, C), (C // 4) ** -0.5, 0.375)
    return {"grid_latents": grid_latents, "mesh_latents": mesh_latents, "neighbour_tiles": neighbour_tiles, "neighbour_live": neighbour_live, "w_query": w_query, "w_keyval": w_keyval, "w_out": w_out}


def attend_tile(query_tile, chosen, live_list):
    model_width = query_tile.shape[1]
    head_size = model_width // HEADS
    key_rows = NB * TILE
    key_part = chosen[:, :, :model_width].reshape(key_rows, HEADS, head_size).astype(jnp.float32)
    value_part = chosen[:, :, model_width:].reshape(key_rows, HEADS, head_size).astype(jnp.float32)
    query_heads = query_tile.reshape(TILE, HEADS, head_size).astype(jnp.float32)
    scores = jnp.einsum('qhd,khd->hqk', query_heads, value_part * 0.0 + key_part) * (head_size ** -0.5)
    key_live = jnp.repeat(live_list > 0, TILE)
    scores = jnp.where(key_live[None, None, :], scores, -1e30)
    row_top = jnp.max(scores, axis=-1, keepdims=True)
    raised = jnp.exp(scores - row_top)
    row_total = jnp.sum(raised, axis=-1, keepdims=True)
    weights = (raised / row_total).astype(jnp.bfloat16)
    mixture = jnp.einsum('hqk,khd->qhd', weights.astype(jnp.float32), value_part)
    return mixture.astype(jnp.bfloat16).reshape(TILE, model_width)


def reference(grid_latents, mesh_latents, neighbour_tiles, neighbour_live, w_query, w_keyval, w_out):
    model_width = w_query.shape[0]
    grid_blocks = grid_latents.reshape(N_NODES, GT_DEV * TILE, model_width)

    def project_block(block):
        return jnp.dot(block, w_keyval, preferred_element_type=jnp.float32).astype(jnp.bfloat16)

    keyval = lax.map(project_block, grid_blocks).reshape(-1, TILE, 2 * model_width)
    queries = jnp.dot(mesh_latents, w_query, preferred_element_type=jnp.float32).astype(jnp.bfloat16)
    queries = queries.reshape(-1, TILE, model_width)

    def one_tile(inputs):
        query_tile, tile_list, live_list = inputs
        chosen = jnp.take(keyval, tile_list.astype(jnp.int32), axis=0)
        return attend_tile(query_tile, chosen, live_list)

    attended = lax.map(one_tile, (queries, neighbour_tiles, neighbour_live))
    attended = attended.reshape(-1, model_width)
    return mesh_latents.astype(jnp.float32) + jnp.dot(attended, w_out, preferred_element_type=jnp.float32)
```

```python
import functools

import jax
import jax.numpy as jnp
from jax import lax
from jax.experimental import pallas as pl
from jax.experimental.pallas import tpu as pltpu
from jax.sharding import PartitionSpec as P


HEADS = 16
TILE = 128
REACH = 2
CAP = 2
LOW = -1e30

SMEM = pl.BlockSpec(memory_space=pltpu.SMEM)
VMEM = pl.BlockSpec(memory_space=pltpu.VMEM)
HBM = pl.BlockSpec(memory_space=pltpu.HBM)
MIB = 1 << 20


def partner_of(i, n):
    return i + 1 - 2 * (i % 2)


def cross_of(i, n):
    return (i + n - 1 + 2 * (i % 2)) % n


def ahead_of(i, n):
    return (i + REACH) % n


def behind_of(i, n):
    return (i + n - REACH) % n


SOURCES = (behind_of, ahead_of, cross_of, partner_of)
STAGES = ((3,), (0, 1))
LAST = 2


def span_of(listed, base, own):
    low = jnp.int32(own)
    high = jnp.int32(-1)
    for entry in listed:
        local = entry - base
        held = (local >= 0) & (local < own)
        low = jnp.minimum(low, jnp.where(held, local, own))
        high = jnp.maximum(high, jnp.where(held, local, -1))
    return low, high


def entries(ref):
    return [ref[i, j] for i in range(ref.shape[0]) for j in range(ref.shape[1])]


def pack_kernel(*refs):
    count = len(SOURCES)
    asked, grid, outs = refs[:count], refs[count], refs[count + 1 :]
    own = grid.shape[0]
    me = lax.axis_index("nodes")
    for c in range(count):
        low, high = span_of(entries(asked[c]), me * own, own)
        low = jnp.where(high < 0, 0, low)
        high = jnp.maximum(high, 0)
        outs[c][0] = grid[low]
        outs[c][1] = grid[high]


def pack(asked, grid):
    count = len(SOURCES)
    shape = jax.ShapeDtypeStruct((CAP,) + grid.shape[1:], grid.dtype)
    return pl.pallas_call(
        pack_kernel,
        out_shape=[shape] * count,
        in_specs=[SMEM] * count + [VMEM],
        out_specs=[VMEM] * count,
        compiler_params=pltpu.CompilerParams(vmem_limit_bytes=4 * MIB),
        name="pack",
    )(*asked, grid)


def project(rows_ref, w_keyval, keys, values, model_width):
    rows = rows_ref.shape[0]
    step = 256
    depth = min(rows, 512)
    for at in range(0, rows, depth):
        block = rows_ref[at : at + depth, :]
        for column in range(0, model_width, step):
            part = jnp.dot(
                block, w_keyval[:, column : column + step], preferred_element_type=jnp.float32
            )
            keys[at : at + depth, column : column + step] = part.astype(jnp.bfloat16)
            part = jnp.dot(
                block,
                w_keyval[:, model_width + column : model_width + column + step],
                preferred_element_type=jnp.float32,
            )
            turned = part.astype(jnp.bfloat16).T
            for k in range(depth // TILE):
                values[at // TILE + k, column : column + step, :] = turned[
                    :, k * TILE : (k + 1) * TILE
                ]


def add_tile(tile, mesh_tile, keys, values, queries, tops, totals, mixed):
    pairs = queries.shape[1]
    width = queries.shape[2]
    head = width // 2
    start = pl.multiple_of(tile * TILE, TILE)
    for pair in range(pairs):
        lanes = slice(pair * width, (pair + 1) * width)
        scores = jnp.dot(
            keys[pl.ds(start, TILE), lanes],
            queries[mesh_tile, pair],
            preferred_element_type=jnp.float32,
        )
        old = tops[mesh_tile, pair : pair + 1, :]
        new = jnp.maximum(old, jnp.max(scores, axis=0, keepdims=True))
        shrink = jnp.exp(old - new)
        raised = jnp.exp(scores - new)
        tops[mesh_tile, pair : pair + 1, :] = new
        totals[mesh_tile, pair : pair + 1, :] = totals[
            mesh_tile, pair : pair + 1, :
        ] * shrink + jnp.sum(raised, axis=0, keepdims=True)
        weights = raised.astype(jnp.bfloat16)
        for k in range(2):
            rows = slice(pair * width + k * head, pair * width + (k + 1) * head)
            cols = slice(k * TILE, (k + 1) * TILE)
            part = jnp.dot(
                values[tile, rows, :], weights[:, cols], preferred_element_type=jnp.float32
            )
            mixed[mesh_tile, rows, :] = mixed[mesh_tile, rows, :] * shrink[:, cols] + part


def lists(tiles_ref, live_ref, mesh_tile, wanted):
    found = jnp.bool_(False)
    for j in range(tiles_ref.shape[1]):
        found = found | ((live_ref[mesh_tile, j] > 0) & (tiles_ref[mesh_tile, j] == wanted))
    return found


def add_listed(count, keep, tiles_ref, live_ref, *state):
    mesh_tiles = tiles_ref.shape[0]

    def body(i, carry):
        tile = i // mesh_tiles
        mesh_tile = i % mesh_tiles
        wanted, fresh = keep(tile)

        @pl.when(fresh & lists(tiles_ref, live_ref, mesh_tile, wanted))
        def _():
            add_tile(tile, mesh_tile, *state)

        return carry

    lax.fori_loop(0, count * mesh_tiles, body, 0)


def front_kernel(mesh_hbm, w_query_hbm, grid_hbm, w_keyval_hbm, queries, grid, w_keyval, mesh, w_query, sems):
    model_width = w_query.shape[0]
    width = queries.shape[2]
    head = width // 2
    step = 256
    copies = [
        pltpu.make_async_copy(source, target, sems.at[k])
        for k, (source, target) in enumerate(
            (
                (mesh_hbm, mesh),
                (w_query_hbm, w_query),
                (grid_hbm, grid),
                (w_keyval_hbm, w_keyval),
            )
        )
    ]
    for copy in copies:
        copy.start()
    queries[...] = jnp.zeros(queries.shape, queries.dtype)
    copies[0].wait()
    copies[1].wait()
    for column in range(0, model_width, step):
        part = jnp.dot(
            mesh[...], w_query[:, column : column + step], preferred_element_type=jnp.float32
        )
        turned = (part.astype(jnp.bfloat16) * jnp.bfloat16(head ** -0.5)).T
        for m in range(queries.shape[0]):
            for h in range(step // head):
                which = column // head + h
                k = which % 2
                queries[m, which // 2, k * head : (k + 1) * head, k * TILE : (k + 1) * TILE] = turned[
                    h * head : (h + 1) * head, m * TILE : (m + 1) * TILE
                ]
    copies[2].wait()
    copies[3].wait()


def own_kernel(tiles_ref, live_ref, grid, w_keyval, queries, tops, totals, mixed, keys, values):
    own = grid.shape[0] // TILE
    tops[...] = jnp.full(tops.shape, LOW, jnp.float32)
    totals[...] = jnp.zeros(totals.shape, jnp.float32)
    mixed[...] = jnp.zeros(mixed.shape, jnp.float32)
    project(grid, w_keyval, keys, values, w_keyval.shape[0])
    base = lax.axis_index("nodes") * own

    def keep(tile):
        return base + tile, jnp.bool_(True)

    add_listed(own, keep, tiles_ref, live_ref, keys, values, queries, tops, totals, mixed)


def chunk_update(sources, own, tiles_ref, live_ref, rows_ref, w_keyval, keys, values, *state):
    me = lax.axis_index("nodes")
    n = lax.axis_size("nodes")
    listed = [
        jnp.where(live > 0, tile, -1)
        for tile, live in zip(entries(tiles_ref), entries(live_ref))
    ]
    project(rows_ref, w_keyval, keys, values, w_keyval.shape[0])
    wanted = []
    for source in sources:
        base = source(me, n) * own
        low, high = span_of(listed, base, own)
        wanted.append(jnp.where(low < own, base + low, -1))
        wanted.append(jnp.where(low < high, base + high, -1))

    def keep(tile):
        found = wanted[0]
        for k in range(1, len(wanted)):
            found = jnp.where(tile == k, wanted[k], found)
        return found, found >= 0

    add_listed(len(wanted), keep, tiles_ref, live_ref, keys, values, *state)


def chunk_kernel(sources, own, tiles_ref, live_ref, w_keyval, queries, tops_in, totals_in, mixed_in, *refs):
    count = len(sources)
    chunks, (tops, totals, mixed, rows, keys, values) = refs[:count], refs[count:]
    tops[...] = tops_in[...]
    totals[...] = totals_in[...]
    mixed[...] = mixed_in[...]
    for k, chunk in enumerate(chunks):
        size = chunk.shape[0]
        rows[k * size : (k + 1) * size, :] = chunk[...]
    chunk_update(sources, own, tiles_ref, live_ref, rows, w_keyval, keys, values, queries, tops, totals, mixed)


def last_kernel(sources, own, tiles_ref, live_ref, w_keyval, queries, tops_in, totals_in, mixed_in, chunk, mesh, w_out, out, tops, totals, mixed, keys, values):
    tops[...] = tops_in[...]
    totals[...] = totals_in[...]
    mixed[...] = mixed_in[...]
    chunk_update(sources, own, tiles_ref, live_ref, chunk, w_keyval, keys, values, queries, tops, totals, mixed)
    pairs = queries.shape[1]
    width = queries.shape[2]
    head = width // 2
    for m in range(queries.shape[0]):
        parts = []
        for pair in range(pairs):
            share = 1.0 / totals[m, pair : pair + 1, :]
            for k in range(2):
                rows = slice(pair * width + k * head, pair * width + (k + 1) * head)
                parts.append(
                    (mixed[m, rows, :] * share[:, k * TILE : (k + 1) * TILE]).astype(jnp.bfloat16)
                )
        attended = jnp.concatenate(parts, axis=0).T
        rows = slice(m * TILE, (m + 1) * TILE)
        out[rows, :] = mesh[rows, :].astype(jnp.float32) + jnp.dot(
            attended, w_out[...], preferred_element_type=jnp.float32
        )


def per_device(
    grid_latents, mesh_latents, neighbour_tiles, neighbour_live, w_query, w_keyval, w_out
):
    model_width = w_query.shape[0]
    own = grid_latents.shape[0] // TILE
    mesh_tiles = mesh_latents.shape[0] // TILE
    n = lax.axis_size("nodes")
    pairs = HEADS // 2
    width = model_width // pairs

    def to_sources(block, source):
        return lax.ppermute(block, "nodes", [(i, source(i, n)) for i in range(n)])

    def from_sources(block, source):
        return lax.ppermute(block, "nodes", [(source(i, n), i) for i in range(n)])

    f32 = jnp.float32
    bf16 = jnp.bfloat16
    stat = jax.ShapeDtypeStruct((mesh_tiles, pairs, 2 * TILE), f32)
    mix = jax.ShapeDtypeStruct((mesh_tiles, model_width, TILE), f32)
    query = jax.ShapeDtypeStruct((mesh_tiles, pairs, width, 2 * TILE), bf16)

    wanted = jnp.where(neighbour_live > 0, neighbour_tiles, -1)
    asked = []
    for source in SOURCES:
        asked.append(to_sources(wanted, source))
    stored = [
        pltpu.with_memory_space_constraint(array, pltpu.HBM)
        for array in (
            mesh_latents,
            w_query,
            grid_latents.reshape(own, TILE, model_width),
            w_keyval,
        )
    ]
    queries, grid, w_kv = pl.pallas_call(
        front_kernel,
        out_shape=[query, jax.ShapeDtypeStruct(stored[2].shape, bf16), jax.ShapeDtypeStruct(w_keyval.shape, bf16)],
        in_specs=[HBM] * 4,
        out_specs=[VMEM] * 3,
        scratch_shapes=[
            pltpu.VMEM(mesh_latents.shape, bf16),
            pltpu.VMEM(w_query.shape, bf16),
            pltpu.SemaphoreType.DMA((4,)),
        ],
        compiler_params=pltpu.CompilerParams(vmem_limit_bytes=8 * MIB),
        cost_estimate=pl.CostEstimate(flops=10**9, transcendentals=0, bytes_accessed=10**7),
        name="front",
    )(*stored)
    packed = pack(asked, grid)
    chunks = []
    for block, source in zip(packed, SOURCES):
        chunks.append(from_sources(block, source).reshape(CAP * TILE, model_width))
    tops, totals, mixed = pl.pallas_call(
        own_kernel,
        out_shape=[stat, stat, mix],
        in_specs=[SMEM, SMEM, VMEM, VMEM, VMEM],
        out_specs=[VMEM] * 3,
        scratch_shapes=[pltpu.VMEM((own * TILE, model_width), bf16), pltpu.VMEM((own, model_width, TILE), bf16)],
        compiler_params=pltpu.CompilerParams(vmem_limit_bytes=16 * MIB),
        cost_estimate=pl.CostEstimate(flops=6 * 10**9, transcendentals=0, bytes_accessed=10**7),
        name="own",
    )(neighbour_tiles, neighbour_live, grid.reshape(own * TILE, model_width), w_kv, queries)

    for members in STAGES:
        sources = [SOURCES[c] for c in members]
        rows = len(members) * CAP * TILE
        tops, totals, mixed = pl.pallas_call(
            functools.partial(chunk_kernel, sources, own),
            out_shape=[stat, stat, mix],
            in_specs=[SMEM, SMEM] + [VMEM] * (5 + len(members)),
            out_specs=[VMEM] * 3,
            scratch_shapes=[
                pltpu.VMEM((rows, model_width), bf16),
                pltpu.VMEM((rows, model_width), bf16),
                pltpu.VMEM((rows // TILE, model_width, TILE), bf16),
            ],
            input_output_aliases={4: 0, 5: 1, 6: 2},
            compiler_params=pltpu.CompilerParams(vmem_limit_bytes=12 * MIB),
            cost_estimate=pl.CostEstimate(flops=2 * 10**9, transcendentals=0, bytes_accessed=10**6),
            name="chunk",
        )(neighbour_tiles, neighbour_live, w_kv, queries, tops, totals, mixed, *[chunks[c] for c in members])
    return pl.pallas_call(
        functools.partial(last_kernel, [SOURCES[LAST]], own),
        out_shape=jax.ShapeDtypeStruct(mesh_latents.shape, f32),
        in_specs=[SMEM, SMEM] + [VMEM] * 8,
        out_specs=VMEM,
        scratch_shapes=[pltpu.VMEM(shape.shape, f32) for shape in (stat, stat, mix)]
        + [
            pltpu.VMEM((CAP * TILE, model_width), bf16),
            pltpu.VMEM((CAP, model_width, TILE), bf16),
        ],
        compiler_params=pltpu.CompilerParams(vmem_limit_bytes=12 * MIB),
        cost_estimate=pl.CostEstimate(flops=3 * 10**9, transcendentals=0, bytes_accessed=10**6),
        name="last",
    )(neighbour_tiles, neighbour_live, w_kv, queries, tops, totals, mixed, chunks[LAST], mesh_latents, w_out)


def solution(mesh):
    return jax.shard_map(
        per_device,
        mesh=mesh,
        in_specs=(
            P(("groups", "nodes"), None),
            P(("groups", "nodes"), None),
            P("nodes", None),
            P("nodes", None),
            P(),
            P(),
            P(),
        ),
        out_specs=P(("groups", "nodes"), None),
        check_vma=False,
    )
```

```python
import functools

import jax
import jax.numpy as jnp
from jax import lax
from jax.experimental import pallas as pl
from jax.experimental.pallas import tpu as pltpu
from jax.sharding import PartitionSpec as P


HEADS = 16
TILE = 128
REACH = 2
CAP = 2
LOW = -1e30

SMEM = pl.BlockSpec(memory_space=pltpu.SMEM)
VMEM = pl.BlockSpec(memory_space=pltpu.VMEM)
HBM = pl.BlockSpec(memory_space=pltpu.HBM)
MIB = 1 << 20


def partner_of(i, n):
    return i + 1 - 2 * (i % 2)


def cross_of(i, n):
    return (i + n - 1 + 2 * (i % 2)) % n


def relay_of(i, n):
    return (i + n - REACH + 2 * REACH * (i % 2)) % n


def ahead_of(i, n):
    return (i + REACH) % n


def behind_of(i, n):
    return (i + n - REACH) % n


SOURCES = (behind_of, ahead_of, cross_of)
STAGES = ((0, 1),)
LAST = 2


def span_of(listed, base, own):
    low = jnp.int32(own)
    high = jnp.int32(-1)
    for entry in listed:
        local = entry - base
        held = (local >= 0) & (local < own)
        low = jnp.minimum(low, jnp.where(held, local, own))
        high = jnp.maximum(high, jnp.where(held, local, -1))
    return low, high


def entries(ref):
    return [ref[i, j] for i in range(ref.shape[0]) for j in range(ref.shape[1])]


def copy_listed(listed, base, grid, out):
    own = grid.shape[0]
    low, high = span_of(listed, base, own)
    out[0] = grid[jnp.where(high < 0, 0, low)]
    out[1] = grid[jnp.maximum(high, 0)]


def pack_kernel(from_ahead, from_behind, grid, to_ahead, to_behind):
    base = lax.axis_index("nodes") * grid.shape[0]
    copy_listed(entries(from_ahead), base, grid, to_ahead)
    copy_listed(entries(from_behind), base, grid, to_behind)


def relay_kernel(from_ahead, from_behind, grid, out):
    me = lax.axis_index("nodes")
    base = partner_of(me, lax.axis_size("nodes")) * grid.shape[0]
    even = me % 2 == 0
    listed = [
        jnp.where(even, ahead, behind)
        for ahead, behind in zip(entries(from_ahead), entries(from_behind))
    ]
    copy_listed(listed, base, grid, out)


def pack(kernel, count, asked, grid):
    shape = jax.ShapeDtypeStruct((CAP,) + grid.shape[1:], grid.dtype)
    return pl.pallas_call(
        kernel,
        out_shape=[shape] * count,
        in_specs=[SMEM, SMEM, VMEM],
        out_specs=[VMEM] * count,
        compiler_params=pltpu.CompilerParams(vmem_limit_bytes=4 * MIB),
    )(*asked, grid)


def project(rows_ref, w_keyval, keys, values, model_width):
    rows = rows_ref.shape[0]
    step = 256
    depth = min(rows, 512)
    for at in range(0, rows, depth):
        block = rows_ref[at : at + depth, :]
        for column in range(0, model_width, step):
            part = jnp.dot(
                block, w_keyval[:, column : column + step], preferred_element_type=jnp.float32
            )
            keys[at : at + depth, column : column + step] = part.astype(jnp.bfloat16)
            part = jnp.dot(
                block,
                w_keyval[:, model_width + column : model_width + column + step],
                preferred_element_type=jnp.float32,
            )
            turned = part.astype(jnp.bfloat16).T
            for k in range(depth // TILE):
                values[at // TILE + k, column : column + step, :] = turned[
                    :, k * TILE : (k + 1) * TILE
                ]


def add_tile(tile, mesh_tile, keys, values, queries, tops, totals, mixed):
    pairs = queries.shape[1]
    width = queries.shape[2]
    head = width // 2
    start = pl.multiple_of(tile * TILE, TILE)
    for pair in range(pairs):
        lanes = slice(pair * width, (pair + 1) * width)
        scores = jnp.dot(
            keys[pl.ds(start, TILE), lanes],
            queries[mesh_tile, pair],
            preferred_element_type=jnp.float32,
        )
        old = tops[mesh_tile, pair : pair + 1, :]
        new = jnp.maximum(old, jnp.max(scores, axis=0, keepdims=True))
        shrink = jnp.exp(old - new)
        raised = jnp.exp(scores - new)
        tops[mesh_tile, pair : pair + 1, :] = new
        totals[mesh_tile, pair : pair + 1, :] = totals[
            mesh_tile, pair : pair + 1, :
        ] * shrink + jnp.sum(raised, axis=0, keepdims=True)
        weights = raised.astype(jnp.bfloat16)
        for k in range(2):
            rows = slice(pair * width + k * head, pair * width + (k + 1) * head)
            cols = slice(k * TILE, (k + 1) * TILE)
            part = jnp.dot(
                values[tile, rows, :], weights[:, cols], preferred_element_type=jnp.float32
            )
            mixed[mesh_tile, rows, :] = mixed[mesh_tile, rows, :] * shrink[:, cols] + part


def lists(tiles_ref, live_ref, mesh_tile, wanted):
    found = jnp.bool_(False)
    for j in range(tiles_ref.shape[1]):
        found = found | ((live_ref[mesh_tile, j] > 0) & (tiles_ref[mesh_tile, j] == wanted))
    return found


def add_listed(count, keep, tiles_ref, live_ref, *state):
    mesh_tiles = tiles_ref.shape[0]

    def body(i, carry):
        tile = i // mesh_tiles
        mesh_tile = i % mesh_tiles
        wanted, fresh = keep(tile)

        @pl.when(fresh & lists(tiles_ref, live_ref, mesh_tile, wanted))
        def _():
            add_tile(tile, mesh_tile, *state)

        return carry

    lax.fori_loop(0, count * mesh_tiles, body, 0)


def front_kernel(mesh_hbm, w_query_hbm, queries, mesh, w_query, sems):
    model_width = w_query.shape[0]
    width = queries.shape[2]
    head = width // 2
    step = 256
    copies = [pltpu.make_async_copy(mesh_hbm, mesh, sems.at[0])]
    for k, column in enumerate(range(0, model_width, step)):
        columns = pl.ds(column, step)
        copies.append(
            pltpu.make_async_copy(w_query_hbm.at[:, columns], w_query.at[:, columns], sems.at[k + 1])
        )
    for copy in copies:
        copy.start()
    queries[...] = jnp.zeros(queries.shape, queries.dtype)
    copies[0].wait()
    for n, column in enumerate(range(0, model_width, step)):
        copies[n + 1].wait()
        part = jnp.dot(
            mesh[...], w_query[:, column : column + step], preferred_element_type=jnp.float32
        )
        turned = (part.astype(jnp.bfloat16) * jnp.bfloat16(head ** -0.5)).T
        for m in range(queries.shape[0]):
            for h in range(step // head):
                which = column // head + h
                k = which % 2
                queries[m, which // 2, k * head : (k + 1) * head, k * TILE : (k + 1) * TILE] = turned[
                    h * head : (h + 1) * head, m * TILE : (m + 1) * TILE
                ]


def own_kernel(tiles_ref, live_ref, grid, beside, w_keyval, queries, tops, totals, mixed, rows, keys, values, found):
    own = grid.shape[0] // TILE
    mesh_tiles = tiles_ref.shape[0]
    tops[...] = jnp.full(tops.shape, LOW, jnp.float32)
    totals[...] = jnp.zeros(totals.shape, jnp.float32)
    mixed[...] = jnp.zeros(mixed.shape, jnp.float32)
    me = lax.axis_index("nodes")
    base = me * own
    base_beside = partner_of(me, lax.axis_size("nodes")) * own
    masks = []
    for m in range(mesh_tiles):
        mask = jnp.int32(0)
        for j in range(tiles_ref.shape[1]):
            tile = tiles_ref[m, j]
            here = tile - base
            there = tile - base_beside
            bit = jnp.where((here >= 0) & (here < own), here, -1)
            bit = jnp.where((there >= 0) & (there < own), there + own, bit)
            taken = (live_ref[m, j] > 0) & (bit >= 0)
            mask = mask | jnp.where(taken, lax.shift_left(jnp.int32(1), jnp.maximum(bit, 0)), 0)
        masks.append(mask)
    union = functools.reduce(jnp.bitwise_or, masks)
    count = jnp.int32(0)
    for bit in range(2 * own):
        found[count] = jnp.int32(bit)
        count = count + ((union >> bit) & 1)
    found[count] = jnp.int32(0)
    group = rows.shape[0] // TILE

    def body(g, carry):
        for k in range(group):
            bit = found[g * group + k]
            place = slice(k * TILE, (k + 1) * TILE)

            @pl.when(bit < own)
            def _():
                rows[place, :] = grid[pl.ds(pl.multiple_of(bit * TILE, TILE), TILE), :]

            @pl.when(bit >= own)
            def _():
                rows[place, :] = beside[pl.ds(pl.multiple_of((bit - own) * TILE, TILE), TILE), :]

        project(rows, w_keyval, keys, values, w_keyval.shape[0])

        def visit(i, inner):
            k = i // mesh_tiles
            m = i % mesh_tiles
            place = g * group + k
            mask = masks[0]
            for other in range(1, mesh_tiles):
                mask = jnp.where(m == other, masks[other], mask)
            taken = (lax.shift_right_logical(mask, found[place]) & 1) > 0

            @pl.when(taken & (place < count))
            def _():
                add_tile(k, m, keys, values, queries, tops, totals, mixed)

            return inner

        return lax.fori_loop(0, group * mesh_tiles, visit, carry)

    lax.fori_loop(0, (count + group - 1) // group, body, 0)


def chunk_update(sources, own, tiles_ref, live_ref, rows_ref, w_keyval, keys, values, *state):
    me = lax.axis_index("nodes")
    n = lax.axis_size("nodes")
    listed = [
        jnp.where(live > 0, tile, -1)
        for tile, live in zip(entries(tiles_ref), entries(live_ref))
    ]
    project(rows_ref, w_keyval, keys, values, w_keyval.shape[0])
    wanted = []
    for source in sources:
        base = source(me, n) * own
        low, high = span_of(listed, base, own)
        wanted.append(jnp.where(low < own, base + low, -1))
        wanted.append(jnp.where(low < high, base + high, -1))

    def keep(tile):
        found = wanted[0]
        for k in range(1, len(wanted)):
            found = jnp.where(tile == k, wanted[k], found)
        return found, found >= 0

    add_listed(len(wanted), keep, tiles_ref, live_ref, keys, values, *state)


def chunk_kernel(sources, own, tiles_ref, live_ref, w_keyval, queries, tops_in, totals_in, mixed_in, *refs):
    count = len(sources)
    chunks, (tops, totals, mixed, rows, keys, values) = refs[:count], refs[count:]
    tops[...] = tops_in[...]
    totals[...] = totals_in[...]
    mixed[...] = mixed_in[...]
    for k, chunk in enumerate(chunks):
        size = chunk.shape[0]
        rows[k * size : (k + 1) * size, :] = chunk[...]
    chunk_update(sources, own, tiles_ref, live_ref, rows, w_keyval, keys, values, queries, tops, totals, mixed)


def last_kernel(sources, own, tiles_ref, live_ref, w_keyval, queries, tops_in, totals_in, mixed_in, chunk, mesh, w_out, out, tops, totals, mixed, keys, values):
    tops[...] = tops_in[...]
    totals[...] = totals_in[...]
    mixed[...] = mixed_in[...]
    chunk_update(sources, own, tiles_ref, live_ref, chunk, w_keyval, keys, values, queries, tops, totals, mixed)
    pairs = queries.shape[1]
    width = queries.shape[2]
    head = width // 2
    for m in range(queries.shape[0]):
        parts = []
        for pair in range(pairs):
            share = 1.0 / totals[m, pair : pair + 1, :]
            for k in range(2):
                rows = slice(pair * width + k * head, pair * width + (k + 1) * head)
                parts.append(
                    (mixed[m, rows, :] * share[:, k * TILE : (k + 1) * TILE]).astype(jnp.bfloat16)
                )
        attended = jnp.concatenate(parts, axis=0).T
        rows = slice(m * TILE, (m + 1) * TILE)
        out[rows, :] = mesh[rows, :].astype(jnp.float32) + jnp.dot(
            attended, w_out[...], preferred_element_type=jnp.float32
        )


def per_device(
    grid_latents, mesh_latents, neighbour_tiles, neighbour_live, w_query, w_keyval, w_out
):
    model_width = w_query.shape[0]
    own = grid_latents.shape[0] // TILE
    mesh_tiles = mesh_latents.shape[0] // TILE
    n = lax.axis_size("nodes")
    pairs = HEADS // 2
    width = model_width // pairs

    def to_sources(block, source):
        return lax.ppermute(block, "nodes", [(i, source(i, n)) for i in range(n)])

    def from_sources(block, source):
        return lax.ppermute(block, "nodes", [(source(i, n), i) for i in range(n)])

    f32 = jnp.float32
    bf16 = jnp.bfloat16
    stat = jax.ShapeDtypeStruct((mesh_tiles, pairs, 2 * TILE), f32)
    mix = jax.ShapeDtypeStruct((mesh_tiles, model_width, TILE), f32)
    query = jax.ShapeDtypeStruct((mesh_tiles, pairs, width, 2 * TILE), bf16)

    wanted = jnp.where(neighbour_live > 0, neighbour_tiles, -1)
    asked = []
    for source in (behind_of, ahead_of):
        asked.append(to_sources(wanted, source))
    tiled = grid_latents.reshape(own, TILE, model_width)
    beside = from_sources(tiled, partner_of)
    stored = [
        pltpu.with_memory_space_constraint(array, pltpu.HBM)
        for array in (mesh_latents, w_query)
    ]
    queries = pl.pallas_call(
        front_kernel,
        out_shape=query,
        in_specs=[HBM] * 2,
        out_specs=VMEM,
        scratch_shapes=[
            pltpu.VMEM(mesh_latents.shape, bf16),
            pltpu.VMEM(w_query.shape, bf16),
            pltpu.SemaphoreType.DMA((1 + model_width // 256,)),
        ],
        compiler_params=pltpu.CompilerParams(vmem_limit_bytes=8 * MIB),
        cost_estimate=pl.CostEstimate(flops=3 * 10**9, transcendentals=0, bytes_accessed=10**7),
        name="front",
    )(*stored)
    packed = pack(pack_kernel, 2, asked, tiled)
    packed += pack(relay_kernel, 1, asked, beside)
    chunks = []
    for block, source in zip(packed, (behind_of, ahead_of, relay_of)):
        chunks.append(from_sources(block, source).reshape(CAP * TILE, model_width))
    tops, totals, mixed = pl.pallas_call(
        own_kernel,
        out_shape=[stat, stat, mix],
        in_specs=[SMEM, SMEM] + [VMEM] * 4,
        out_specs=[VMEM] * 3,
        scratch_shapes=[
            pltpu.VMEM((CAP * TILE, model_width), bf16),
            pltpu.VMEM((CAP * TILE, model_width), bf16),
            pltpu.VMEM((CAP, model_width, TILE), bf16),
            pltpu.SMEM((2 * own + 1,), jnp.int32),
        ],
        compiler_params=pltpu.CompilerParams(vmem_limit_bytes=12 * MIB),
        cost_estimate=pl.CostEstimate(flops=6 * 10**9, transcendentals=0, bytes_accessed=10**7),
        name="own",
    )(
        neighbour_tiles,
        neighbour_live,
        grid_latents,
        beside.reshape(own * TILE, model_width),
        w_keyval,
        queries,
    )

    for members in STAGES:
        sources = [SOURCES[c] for c in members]
        rows = len(members) * CAP * TILE
        tops, totals, mixed = pl.pallas_call(
            functools.partial(chunk_kernel, sources, own),
            out_shape=[stat, stat, mix],
            in_specs=[SMEM, SMEM] + [VMEM] * (5 + len(members)),
            out_specs=[VMEM] * 3,
            scratch_shapes=[
                pltpu.VMEM((rows, model_width), bf16),
                pltpu.VMEM((rows, model_width), bf16),
                pltpu.VMEM((rows // TILE, model_width, TILE), bf16),
            ],
            input_output_aliases={4: 0, 5: 1, 6: 2},
            compiler_params=pltpu.CompilerParams(vmem_limit_bytes=12 * MIB),
            cost_estimate=pl.CostEstimate(flops=2 * 10**9, transcendentals=0, bytes_accessed=10**6),
            name="chunk",
        )(neighbour_tiles, neighbour_live, w_keyval, queries, tops, totals, mixed, *[chunks[c] for c in members])
    return pl.pallas_call(
        functools.partial(last_kernel, [SOURCES[LAST]], own),
        out_shape=jax.ShapeDtypeStruct(mesh_latents.shape, f32),
        in_specs=[SMEM, SMEM] + [VMEM] * 8,
        out_specs=VMEM,
        scratch_shapes=[pltpu.VMEM(shape.shape, f32) for shape in (stat, stat, mix)]
        + [
            pltpu.VMEM((CAP * TILE, model_width), bf16),
            pltpu.VMEM((CAP, model_width, TILE), bf16),
        ],
        compiler_params=pltpu.CompilerParams(vmem_limit_bytes=12 * MIB),
        cost_estimate=pl.CostEstimate(flops=3 * 10**9, transcendentals=0, bytes_accessed=10**6),
        name="last",
    )(neighbour_tiles, neighbour_live, w_keyval, queries, tops, totals, mixed, chunks[LAST], mesh_latents, w_out)


def solution(mesh):
    return jax.shard_map(
        per_device,
        mesh=mesh,
        in_specs=(
            P(("groups", "nodes"), None),
            P(("groups", "nodes"), None),
            P("nodes", None),
            P("nodes", None),
            P(),
            P(),
            P(),
        ),
        out_specs=P(("groups", "nodes"), None),
        check_vma=False,
    )
```

```python
import functools

import jax
import jax.numpy as jnp
from jax import lax
from jax.experimental import pallas as pl
from jax.experimental.pallas import tpu as pltpu
from jax.sharding import PartitionSpec as P


HEADS = 16
TILE = 128
REACH = 2
CAP = 2
LOW = -1e30

SMEM = pl.BlockSpec(memory_space=pltpu.SMEM)
VMEM = pl.BlockSpec(memory_space=pltpu.VMEM)
HBM = pl.BlockSpec(memory_space=pltpu.HBM)
MIB = 1 << 20


def partner_of(i, n):
    return i + 1 - 2 * (i % 2)


def cross_of(i, n):
    return (i + n - 1 + 2 * (i % 2)) % n


def relay_of(i, n):
    return (i + n - REACH + 2 * REACH * (i % 2)) % n


def ahead_of(i, n):
    return (i + REACH) % n


def behind_of(i, n):
    return (i + n - REACH) % n


SOURCES = (behind_of, ahead_of, cross_of)
STAGES = ((0, 1),)
LAST = 2


def span_of(listed, base, own):
    low = jnp.int32(own)
    high = jnp.int32(-1)
    for entry in listed:
        local = entry - base
        held = (local >= 0) & (local < own)
        low = jnp.minimum(low, jnp.where(held, local, own))
        high = jnp.maximum(high, jnp.where(held, local, -1))
    return low, high


def entries(ref):
    return [ref[i, j] for i in range(ref.shape[0]) for j in range(ref.shape[1])]


def copy_listed(listed, base, grid, out):
    own = grid.shape[0]
    low, high = span_of(listed, base, own)
    out[0] = grid[jnp.where(high < 0, 0, low)]
    out[1] = grid[jnp.maximum(high, 0)]


def pack_kernel(from_ahead, from_behind, grid, to_ahead, to_behind):
    base = lax.axis_index("nodes") * grid.shape[0]
    copy_listed(entries(from_ahead), base, grid, to_ahead)
    copy_listed(entries(from_behind), base, grid, to_behind)


def relay_kernel(from_ahead, from_behind, grid, out):
    me = lax.axis_index("nodes")
    base = partner_of(me, lax.axis_size("nodes")) * grid.shape[0]
    even = me % 2 == 0
    listed = [
        jnp.where(even, ahead, behind)
        for ahead, behind in zip(entries(from_ahead), entries(from_behind))
    ]
    copy_listed(listed, base, grid, out)


def pack(kernel, count, asked, grid):
    shape = jax.ShapeDtypeStruct((CAP,) + grid.shape[1:], grid.dtype)
    return pl.pallas_call(
        kernel,
        out_shape=[shape] * count,
        in_specs=[SMEM, SMEM, VMEM],
        out_specs=[VMEM] * count,
        compiler_params=pltpu.CompilerParams(vmem_limit_bytes=4 * MIB),
        cost_estimate=pl.CostEstimate(flops=2 * 10**9, transcendentals=0, bytes_accessed=10**6),
    )(*asked, grid)


def project(rows_ref, w_keyval, keys, values, model_width):
    rows = rows_ref.shape[0]
    step = 256
    depth = min(rows, 512)
    for at in range(0, rows, depth):
        block = rows_ref[at : at + depth, :]
        for column in range(0, model_width, step):
            part = jnp.dot(
                block, w_keyval[:, column : column + step], preferred_element_type=jnp.float32
            )
            keys[at : at + depth, column : column + step] = part.astype(jnp.bfloat16)
            part = jnp.dot(
                block,
                w_keyval[:, model_width + column : model_width + column + step],
                preferred_element_type=jnp.float32,
            )
            turned = part.astype(jnp.bfloat16).T
            for k in range(depth // TILE):
                values[at // TILE + k, column : column + step, :] = turned[
                    :, k * TILE : (k + 1) * TILE
                ]


def add_tile(tile, mesh_tile, keys, values, queries, tops, totals, mixed):
    pairs = queries.shape[1]
    width = queries.shape[2]
    head = width // 2
    start = pl.multiple_of(tile * TILE, TILE)
    for pair in range(pairs):
        lanes = slice(pair * width, (pair + 1) * width)
        scores = jnp.dot(
            keys[pl.ds(start, TILE), lanes],
            queries[mesh_tile, pair],
            preferred_element_type=jnp.float32,
        )
        old = tops[mesh_tile, pair : pair + 1, :]
        new = jnp.maximum(old, jnp.max(scores, axis=0, keepdims=True))
        shrink = jnp.exp(old - new)
        raised = jnp.exp(scores - new)
        tops[mesh_tile, pair : pair + 1, :] = new
        totals[mesh_tile, pair : pair + 1, :] = totals[
            mesh_tile, pair : pair + 1, :
        ] * shrink + jnp.sum(raised, axis=0, keepdims=True)
        weights = raised.astype(jnp.bfloat16)
        for k in range(2):
            rows = slice(pair * width + k * head, pair * width + (k + 1) * head)
            cols = slice(k * TILE, (k + 1) * TILE)
            part = jnp.dot(
                values[tile, rows, :], weights[:, cols], preferred_element_type=jnp.float32
            )
            mixed[mesh_tile, rows, :] = mixed[mesh_tile, rows, :] * shrink[:, cols] + part


def lists(tiles_ref, live_ref, mesh_tile, wanted):
    found = jnp.bool_(False)
    for j in range(tiles_ref.shape[1]):
        found = found | ((live_ref[mesh_tile, j] > 0) & (tiles_ref[mesh_tile, j] == wanted))
    return found


def add_listed(count, keep, tiles_ref, live_ref, *state):
    mesh_tiles = tiles_ref.shape[0]

    def body(i, carry):
        tile = i // mesh_tiles
        mesh_tile = i % mesh_tiles
        wanted, fresh = keep(tile)

        @pl.when(fresh & lists(tiles_ref, live_ref, mesh_tile, wanted))
        def _():
            add_tile(tile, mesh_tile, *state)

        return carry

    lax.fori_loop(0, count * mesh_tiles, body, 0)


def front_kernel(grid_hbm, grid, sems):
    half = grid.shape[0] // 2
    copies = [
        pltpu.make_async_copy(
            grid_hbm.at[pl.ds(k * half, half)], grid.at[pl.ds(k * half, half)], sems.at[k]
        )
        for k in range(2)
    ]
    for copy in copies:
        copy.start()
    for copy in copies:
        copy.wait()


def form_queries(mesh, w_query, queries):
    model_width = w_query.shape[0]
    head = queries.shape[2] // 2
    step = 256
    queries[...] = jnp.zeros(queries.shape, queries.dtype)
    for column in range(0, model_width, step):
        part = jnp.dot(
            mesh[...], w_query[:, column : column + step], preferred_element_type=jnp.float32
        )
        turned = (part.astype(jnp.bfloat16) * jnp.bfloat16(head ** -0.5)).T
        for m in range(queries.shape[0]):
            for h in range(step // head):
                which = column // head + h
                k = which % 2
                queries[m, which // 2, k * head : (k + 1) * head, k * TILE : (k + 1) * TILE] = turned[
                    h * head : (h + 1) * head, m * TILE : (m + 1) * TILE
                ]


def own_kernel(tiles_ref, live_ref, grid, beside, w_keyval, mesh, w_query, queries, tops, totals, mixed, rows, keys, values, found):
    own = grid.shape[0] // TILE
    mesh_tiles = tiles_ref.shape[0]
    form_queries(mesh, w_query, queries)
    tops[...] = jnp.full(tops.shape, LOW, jnp.float32)
    totals[...] = jnp.zeros(totals.shape, jnp.float32)
    mixed[...] = jnp.zeros(mixed.shape, jnp.float32)
    me = lax.axis_index("nodes")
    base = me * own
    base_beside = partner_of(me, lax.axis_size("nodes")) * own
    masks = []
    for m in range(mesh_tiles):
        mask = jnp.int32(0)
        for j in range(tiles_ref.shape[1]):
            tile = tiles_ref[m, j]
            here = tile - base
            there = tile - base_beside
            bit = jnp.where((here >= 0) & (here < own), here, -1)
            bit = jnp.where((there >= 0) & (there < own), there + own, bit)
            taken = (live_ref[m, j] > 0) & (bit >= 0)
            mask = mask | jnp.where(taken, lax.shift_left(jnp.int32(1), jnp.maximum(bit, 0)), 0)
        masks.append(mask)
    union = functools.reduce(jnp.bitwise_or, masks)
    count = jnp.int32(0)
    for bit in range(2 * own):
        found[count] = jnp.int32(bit)
        count = count + ((union >> bit) & 1)
    found[count] = jnp.int32(0)
    group = rows.shape[0] // TILE

    def body(g, carry):
        for k in range(group):
            bit = found[g * group + k]
            place = slice(k * TILE, (k + 1) * TILE)

            @pl.when(bit < own)
            def _():
                rows[place, :] = grid[pl.ds(pl.multiple_of(bit * TILE, TILE), TILE), :]

            @pl.when(bit >= own)
            def _():
                rows[place, :] = beside[pl.ds(pl.multiple_of((bit - own) * TILE, TILE), TILE), :]

        project(rows, w_keyval, keys, values, w_keyval.shape[0])

        def visit(i, inner):
            k = i // mesh_tiles
            m = i % mesh_tiles
            place = g * group + k
            mask = masks[0]
            for other in range(1, mesh_tiles):
                mask = jnp.where(m == other, masks[other], mask)
            taken = (lax.shift_right_logical(mask, found[place]) & 1) > 0

            @pl.when(taken & (place < count))
            def _():
                add_tile(k, m, keys, values, queries, tops, totals, mixed)

            return inner

        return lax.fori_loop(0, group * mesh_tiles, visit, carry)

    lax.fori_loop(0, (count + group - 1) // group, body, 0)


def chunk_update(sources, own, tiles_ref, live_ref, rows_ref, w_keyval, keys, values, *state):
    me = lax.axis_index("nodes")
    n = lax.axis_size("nodes")
    listed = [
        jnp.where(live > 0, tile, -1)
        for tile, live in zip(entries(tiles_ref), entries(live_ref))
    ]
    project(rows_ref, w_keyval, keys, values, w_keyval.shape[0])
    wanted = []
    for source in sources:
        base = source(me, n) * own
        low, high = span_of(listed, base, own)
        wanted.append(jnp.where(low < own, base + low, -1))
        wanted.append(jnp.where(low < high, base + high, -1))

    def keep(tile):
        found = wanted[0]
        for k in range(1, len(wanted)):
            found = jnp.where(tile == k, wanted[k], found)
        return found, found >= 0

    add_listed(len(wanted), keep, tiles_ref, live_ref, keys, values, *state)


def chunk_kernel(sources, own, tiles_ref, live_ref, w_keyval, queries, tops_in, totals_in, mixed_in, *refs):
    count = len(sources)
    chunks, (tops, totals, mixed, rows, keys, values) = refs[:count], refs[count:]
    tops[...] = tops_in[...]
    totals[...] = totals_in[...]
    mixed[...] = mixed_in[...]
    for k, chunk in enumerate(chunks):
        size = chunk.shape[0]
        rows[k * size : (k + 1) * size, :] = chunk[...]
    chunk_update(sources, own, tiles_ref, live_ref, rows, w_keyval, keys, values, queries, tops, totals, mixed)


def last_kernel(sources, own, tiles_ref, live_ref, w_keyval, queries, tops_in, totals_in, mixed_in, chunk, mesh, w_out, out, tops, totals, mixed, keys, values):
    tops[...] = tops_in[...]
    totals[...] = totals_in[...]
    mixed[...] = mixed_in[...]
    chunk_update(sources, own, tiles_ref, live_ref, chunk, w_keyval, keys, values, queries, tops, totals, mixed)
    pairs = queries.shape[1]
    width = queries.shape[2]
    head = width // 2
    for m in range(queries.shape[0]):
        parts = []
        for pair in range(pairs):
            share = 1.0 / totals[m, pair : pair + 1, :]
            for k in range(2):
                rows = slice(pair * width + k * head, pair * width + (k + 1) * head)
                parts.append(
                    (mixed[m, rows, :] * share[:, k * TILE : (k + 1) * TILE]).astype(jnp.bfloat16)
                )
        attended = jnp.concatenate(parts, axis=0).T
        rows = slice(m * TILE, (m + 1) * TILE)
        out[rows, :] = mesh[rows, :].astype(jnp.float32) + jnp.dot(
            attended, w_out[...], preferred_element_type=jnp.float32
        )


def per_device(
    grid_latents, mesh_latents, neighbour_tiles, neighbour_live, w_query, w_keyval, w_out
):
    model_width = w_query.shape[0]
    own = grid_latents.shape[0] // TILE
    mesh_tiles = mesh_latents.shape[0] // TILE
    n = lax.axis_size("nodes")
    pairs = HEADS // 2
    width = model_width // pairs

    def to_sources(block, source):
        return lax.ppermute(block, "nodes", [(i, source(i, n)) for i in range(n)])

    def from_sources(block, source):
        return lax.ppermute(block, "nodes", [(source(i, n), i) for i in range(n)])

    f32 = jnp.float32
    bf16 = jnp.bfloat16
    stat = jax.ShapeDtypeStruct((mesh_tiles, pairs, 2 * TILE), f32)
    mix = jax.ShapeDtypeStruct((mesh_tiles, model_width, TILE), f32)
    query = jax.ShapeDtypeStruct((mesh_tiles, pairs, width, 2 * TILE), bf16)

    wanted = jnp.where(neighbour_live > 0, neighbour_tiles, -1)
    asked = []
    for source in (behind_of, ahead_of):
        asked.append(to_sources(wanted, source))
    tiled = grid_latents.reshape(own, TILE, model_width)
    beside = from_sources(tiled, partner_of)
    stored = pltpu.with_memory_space_constraint(tiled, pltpu.HBM)
    near = pl.pallas_call(
        front_kernel,
        out_shape=jax.ShapeDtypeStruct(tiled.shape, bf16),
        in_specs=[HBM],
        out_specs=VMEM,
        scratch_shapes=[pltpu.SemaphoreType.DMA((2,))],
        compiler_params=pltpu.CompilerParams(vmem_limit_bytes=4 * MIB),
        cost_estimate=pl.CostEstimate(flops=10**8, transcendentals=0, bytes_accessed=10**6),
        name="front",
    )(stored)
    packed = pack(pack_kernel, 2, asked, near)
    packed += pack(relay_kernel, 1, asked, beside)
    chunks = []
    for block, source in zip(packed, (behind_of, ahead_of, relay_of)):
        chunks.append(from_sources(block, source).reshape(CAP * TILE, model_width))
    queries, tops, totals, mixed = pl.pallas_call(
        own_kernel,
        out_shape=[query, stat, stat, mix],
        in_specs=[SMEM, SMEM] + [VMEM] * 5,
        out_specs=[VMEM] * 4,
        scratch_shapes=[
            pltpu.VMEM((CAP * TILE, model_width), bf16),
            pltpu.VMEM((CAP * TILE, model_width), bf16),
            pltpu.VMEM((CAP, model_width, TILE), bf16),
            pltpu.SMEM((2 * own + 1,), jnp.int32),
        ],
        compiler_params=pltpu.CompilerParams(vmem_limit_bytes=12 * MIB),
        cost_estimate=pl.CostEstimate(flops=6 * 10**9, transcendentals=0, bytes_accessed=10**7),
        name="own",
    )(
        neighbour_tiles,
        neighbour_live,
        near.reshape(own * TILE, model_width),
        beside.reshape(own * TILE, model_width),
        w_keyval,
        mesh_latents,
        w_query,
    )

    for members in STAGES:
        sources = [SOURCES[c] for c in members]
        rows = len(members) * CAP * TILE
        tops, totals, mixed = pl.pallas_call(
            functools.partial(chunk_kernel, sources, own),
            out_shape=[stat, stat, mix],
            in_specs=[SMEM, SMEM] + [VMEM] * (5 + len(members)),
            out_specs=[VMEM] * 3,
            scratch_shapes=[
                pltpu.VMEM((rows, model_width), bf16),
                pltpu.VMEM((rows, model_width), bf16),
                pltpu.VMEM((rows // TILE, model_width, TILE), bf16),
            ],
            input_output_aliases={4: 0, 5: 1, 6: 2},
            compiler_params=pltpu.CompilerParams(vmem_limit_bytes=12 * MIB),
            cost_estimate=pl.CostEstimate(flops=2 * 10**9, transcendentals=0, bytes_accessed=10**6),
            name="chunk",
        )(neighbour_tiles, neighbour_live, w_keyval, queries, tops, totals, mixed, *[chunks[c] for c in members])
    return pl.pallas_call(
        functools.partial(last_kernel, [SOURCES[LAST]], own),
        out_shape=jax.ShapeDtypeStruct(mesh_latents.shape, f32),
        in_specs=[SMEM, SMEM] + [VMEM] * 8,
        out_specs=VMEM,
        scratch_shapes=[pltpu.VMEM(shape.shape, f32) for shape in (stat, stat, mix)]
        + [
            pltpu.VMEM((CAP * TILE, model_width), bf16),
            pltpu.VMEM((CAP, model_width, TILE), bf16),
        ],
        compiler_params=pltpu.CompilerParams(vmem_limit_bytes=12 * MIB),
        cost_estimate=pl.CostEstimate(flops=3 * 10**9, transcendentals=0, bytes_accessed=10**6),
        name="last",
    )(neighbour_tiles, neighbour_live, w_keyval, queries, tops, totals, mixed, chunks[LAST], mesh_latents, w_out)


def solution(mesh):
    return jax.shard_map(
        per_device,
        mesh=mesh,
        in_specs=(
            P(("groups", "nodes"), None),
            P(("groups", "nodes"), None),
            P("nodes", None),
            P("nodes", None),
            P(),
            P(),
            P(),
        ),
        out_specs=P(("groups", "nodes"), None),
        check_vma=False,
    )
```

```python
import functools

import jax
import jax.numpy as jnp
from jax import lax
from jax.experimental import pallas as pl
from jax.experimental.pallas import tpu as pltpu
from jax.sharding import PartitionSpec as P


HEADS = 16
TILE = 128
REACH = 2
CAP = 2
LOW = -1e30

SMEM = pl.BlockSpec(memory_space=pltpu.SMEM)
VMEM = pl.BlockSpec(memory_space=pltpu.VMEM)
HBM = pl.BlockSpec(memory_space=pltpu.HBM)
MIB = 1 << 20


def partner_of(i, n):
    return i + 1 - 2 * (i % 2)


def cross_of(i, n):
    return (i + n - 1 + 2 * (i % 2)) % n


def relay_of(i, n):
    return (i + n - REACH + 2 * REACH * (i % 2)) % n


def ahead_of(i, n):
    return (i + REACH) % n


def behind_of(i, n):
    return (i + n - REACH) % n


SOURCES = (behind_of, ahead_of, cross_of)
STAGES = (0, 1)
LAST = 2


def span_of(listed, base, own):
    low = jnp.int32(own)
    high = jnp.int32(-1)
    for entry in listed:
        local = entry - base
        held = (local >= 0) & (local < own)
        low = jnp.minimum(low, jnp.where(held, local, own))
        high = jnp.maximum(high, jnp.where(held, local, -1))
    return low, high


def entries(ref):
    return [ref[i, j] for i in range(ref.shape[0]) for j in range(ref.shape[1])]


def copy_listed(listed, base, grid, out):
    own = grid.shape[0]
    low, high = span_of(listed, base, own)
    out[0] = grid[jnp.where(high < 0, 0, low)]
    out[1] = grid[jnp.maximum(high, 0)]


def pack_kernel(from_ahead, from_behind, grid, to_ahead, to_behind):
    base = lax.axis_index("nodes") * grid.shape[0]
    copy_listed(entries(from_ahead), base, grid, to_ahead)
    copy_listed(entries(from_behind), base, grid, to_behind)


def relay_kernel(from_ahead, from_behind, grid, out):
    me = lax.axis_index("nodes")
    base = partner_of(me, lax.axis_size("nodes")) * grid.shape[0]
    even = me % 2 == 0
    listed = [
        jnp.where(even, ahead, behind)
        for ahead, behind in zip(entries(from_ahead), entries(from_behind))
    ]
    copy_listed(listed, base, grid, out)


def pack(kernel, count, asked, grid):
    shape = jax.ShapeDtypeStruct((CAP,) + grid.shape[1:], grid.dtype)
    return pl.pallas_call(
        kernel,
        out_shape=[shape] * count,
        in_specs=[SMEM, SMEM, VMEM],
        out_specs=[VMEM] * count,
        compiler_params=pltpu.CompilerParams(vmem_limit_bytes=4 * MIB),
        cost_estimate=pl.CostEstimate(flops=2 * 10**9, transcendentals=0, bytes_accessed=10**6),
    )(*asked, grid)


def project(rows_ref, w_keyval, keys, values, model_width):
    rows = rows_ref.shape[0]
    step = 256
    depth = min(rows, 512)
    for at in range(0, rows, depth):
        block = rows_ref[at : at + depth, :]
        for column in range(0, model_width, step):
            part = jnp.dot(
                block, w_keyval[:, column : column + step], preferred_element_type=jnp.float32
            )
            keys[at : at + depth, column : column + step] = part.astype(jnp.bfloat16)
            part = jnp.dot(
                block,
                w_keyval[:, model_width + column : model_width + column + step],
                preferred_element_type=jnp.float32,
            )
            turned = part.astype(jnp.bfloat16).T
            for k in range(depth // TILE):
                values[at // TILE + k, column : column + step, :] = turned[
                    :, k * TILE : (k + 1) * TILE
                ]


def add_tile(tile, mesh_tile, keys, values, queries, tops, totals, mixed):
    pairs = queries.shape[1]
    width = queries.shape[2]
    head = width // 2
    start = pl.multiple_of(tile * TILE, TILE)
    for pair in range(pairs):
        lanes = slice(pair * width, (pair + 1) * width)
        scores = jnp.dot(
            keys[pl.ds(start, TILE), lanes],
            queries[mesh_tile, pair],
            preferred_element_type=jnp.float32,
        )
        old = tops[mesh_tile, pair : pair + 1, :]
        new = jnp.maximum(old, jnp.max(scores, axis=0, keepdims=True))
        shrink = jnp.exp(old - new)
        raised = jnp.exp(scores - new)
        tops[mesh_tile, pair : pair + 1, :] = new
        totals[mesh_tile, pair : pair + 1, :] = totals[
            mesh_tile, pair : pair + 1, :
        ] * shrink + jnp.sum(raised, axis=0, keepdims=True)
        weights = raised.astype(jnp.bfloat16)
        for k in range(2):
            rows = slice(pair * width + k * head, pair * width + (k + 1) * head)
            cols = slice(k * TILE, (k + 1) * TILE)
            part = jnp.dot(
                values[tile, rows, :], weights[:, cols], preferred_element_type=jnp.float32
            )
            mixed[mesh_tile, rows, :] = mixed[mesh_tile, rows, :] * shrink[:, cols] + part


def lists(tiles_ref, live_ref, mesh_tile, wanted):
    found = jnp.bool_(False)
    for j in range(tiles_ref.shape[1]):
        found = found | ((live_ref[mesh_tile, j] > 0) & (tiles_ref[mesh_tile, j] == wanted))
    return found


def add_listed(count, keep, tiles_ref, live_ref, *state):
    mesh_tiles = tiles_ref.shape[0]

    def body(i, carry):
        tile = i // mesh_tiles
        mesh_tile = i % mesh_tiles
        wanted, fresh = keep(tile)

        @pl.when(fresh & lists(tiles_ref, live_ref, mesh_tile, wanted))
        def _():
            add_tile(tile, mesh_tile, *state)

        return carry

    lax.fori_loop(0, count * mesh_tiles, body, 0)


def front_kernel(grid_hbm, grid, sems):
    half = grid.shape[0] // 2
    copies = [
        pltpu.make_async_copy(
            grid_hbm.at[pl.ds(k * half, half)], grid.at[pl.ds(k * half, half)], sems.at[k]
        )
        for k in range(2)
    ]
    for copy in copies:
        copy.start()
    for copy in copies:
        copy.wait()


def form_queries(mesh, w_query, queries):
    model_width = w_query.shape[0]
    head = queries.shape[2] // 2
    step = 256
    queries[...] = jnp.zeros(queries.shape, queries.dtype)
    for column in range(0, model_width, step):
        part = jnp.dot(
            mesh[...], w_query[:, column : column + step], preferred_element_type=jnp.float32
        )
        turned = (part.astype(jnp.bfloat16) * jnp.bfloat16(head ** -0.5)).T
        for m in range(queries.shape[0]):
            for h in range(step // head):
                which = column // head + h
                k = which % 2
                queries[m, which // 2, k * head : (k + 1) * head, k * TILE : (k + 1) * TILE] = turned[
                    h * head : (h + 1) * head, m * TILE : (m + 1) * TILE
                ]


def own_kernel(tiles_ref, live_ref, grid, beside, w_keyval, mesh, w_query, queries, tops, totals, mixed, rows, keys, values, found):
    own = grid.shape[0] // TILE
    mesh_tiles = tiles_ref.shape[0]
    form_queries(mesh, w_query, queries)
    tops[...] = jnp.full(tops.shape, LOW, jnp.float32)
    totals[...] = jnp.zeros(totals.shape, jnp.float32)
    mixed[...] = jnp.zeros(mixed.shape, jnp.float32)
    me = lax.axis_index("nodes")
    base = me * own
    base_beside = partner_of(me, lax.axis_size("nodes")) * own
    masks = []
    for m in range(mesh_tiles):
        mask = jnp.int32(0)
        for j in range(tiles_ref.shape[1]):
            tile = tiles_ref[m, j]
            here = tile - base
            there = tile - base_beside
            bit = jnp.where((here >= 0) & (here < own), here, -1)
            bit = jnp.where((there >= 0) & (there < own), there + own, bit)
            taken = (live_ref[m, j] > 0) & (bit >= 0)
            mask = mask | jnp.where(taken, lax.shift_left(jnp.int32(1), jnp.maximum(bit, 0)), 0)
        masks.append(mask)
    union = functools.reduce(jnp.bitwise_or, masks)
    count = jnp.int32(0)
    for bit in range(2 * own):
        found[count] = jnp.int32(bit)
        count = count + ((union >> bit) & 1)
    found[count] = jnp.int32(0)
    group = rows.shape[0] // TILE

    def body(g, carry):
        for k in range(group):
            bit = found[g * group + k]
            place = slice(k * TILE, (k + 1) * TILE)

            @pl.when(bit < own)
            def _():
                rows[place, :] = grid[pl.ds(pl.multiple_of(bit * TILE, TILE), TILE), :]

            @pl.when(bit >= own)
            def _():
                rows[place, :] = beside[pl.ds(pl.multiple_of((bit - own) * TILE, TILE), TILE), :]

        project(rows, w_keyval, keys, values, w_keyval.shape[0])

        def visit(i, inner):
            k = i // mesh_tiles
            m = i % mesh_tiles
            place = g * group + k
            mask = masks[0]
            for other in range(1, mesh_tiles):
                mask = jnp.where(m == other, masks[other], mask)
            taken = (lax.shift_right_logical(mask, found[place]) & 1) > 0

            @pl.when(taken & (place < count))
            def _():
                add_tile(k, m, keys, values, queries, tops, totals, mixed)

            return inner

        return lax.fori_loop(0, group * mesh_tiles, visit, carry)

    lax.fori_loop(0, (count + group - 1) // group, body, 0)


def chunk_update(source, own, tiles_ref, live_ref, rows, w_keyval, keys, values, *state):
    me = lax.axis_index("nodes")
    n = lax.axis_size("nodes")
    listed = [
        jnp.where(live > 0, tile, -1)
        for tile, live in zip(entries(tiles_ref), entries(live_ref))
    ]
    base = source(me, n) * own
    low, high = span_of(listed, base, own)
    wanted = (base + low, jnp.where(low < high, base + high, -1))

    def keep(tile):
        found = jnp.where(tile == 0, wanted[0], wanted[1])
        return found, found >= 0

    @pl.when(high >= 0)
    def _():
        project(rows, w_keyval, keys, values, w_keyval.shape[0])
        add_listed(CAP, keep, tiles_ref, live_ref, keys, values, *state)


def chunk_kernel(source, own, tiles_ref, live_ref, w_keyval, queries, tops_in, totals_in, mixed_in, chunk, tops, totals, mixed, keys, values):
    tops[...] = tops_in[...]
    totals[...] = totals_in[...]
    mixed[...] = mixed_in[...]
    chunk_update(source, own, tiles_ref, live_ref, chunk, w_keyval, keys, values, queries, tops, totals, mixed)


def last_kernel(source, own, tiles_ref, live_ref, w_keyval, queries, tops_in, totals_in, mixed_in, chunk, mesh, w_out, out, tops, totals, mixed, keys, values):
    tops[...] = tops_in[...]
    totals[...] = totals_in[...]
    mixed[...] = mixed_in[...]
    chunk_update(source, own, tiles_ref, live_ref, chunk, w_keyval, keys, values, queries, tops, totals, mixed)
    pairs = queries.shape[1]
    width = queries.shape[2]
    head = width // 2
    for m in range(queries.shape[0]):
        parts = []
        for pair in range(pairs):
            share = 1.0 / totals[m, pair : pair + 1, :]
            for k in range(2):
                rows = slice(pair * width + k * head, pair * width + (k + 1) * head)
                parts.append(
                    (mixed[m, rows, :] * share[:, k * TILE : (k + 1) * TILE]).astype(jnp.bfloat16)
                )
        attended = jnp.concatenate(parts, axis=0).T
        rows = slice(m * TILE, (m + 1) * TILE)
        out[rows, :] = mesh[rows, :].astype(jnp.float32) + jnp.dot(
            attended, w_out[...], preferred_element_type=jnp.float32
        )


def per_device(
    grid_latents, mesh_latents, neighbour_tiles, neighbour_live, w_query, w_keyval, w_out
):
    model_width = w_query.shape[0]
    own = grid_latents.shape[0] // TILE
    mesh_tiles = mesh_latents.shape[0] // TILE
    n = lax.axis_size("nodes")
    pairs = HEADS // 2
    width = model_width // pairs

    def to_sources(block, source):
        return lax.ppermute(block, "nodes", [(i, source(i, n)) for i in range(n)])

    def from_sources(block, source):
        return lax.ppermute(block, "nodes", [(source(i, n), i) for i in range(n)])

    f32 = jnp.float32
    bf16 = jnp.bfloat16
    stat = jax.ShapeDtypeStruct((mesh_tiles, pairs, 2 * TILE), f32)
    mix = jax.ShapeDtypeStruct((mesh_tiles, model_width, TILE), f32)
    query = jax.ShapeDtypeStruct((mesh_tiles, pairs, width, 2 * TILE), bf16)

    wanted = jnp.where(neighbour_live > 0, neighbour_tiles, -1)
    asked = []
    for source in (behind_of, ahead_of):
        asked.append(to_sources(wanted, source))
    tiled = grid_latents.reshape(own, TILE, model_width)
    beside = from_sources(tiled, partner_of)
    stored = pltpu.with_memory_space_constraint(tiled, pltpu.HBM)
    near = pl.pallas_call(
        front_kernel,
        out_shape=jax.ShapeDtypeStruct(tiled.shape, bf16),
        in_specs=[HBM],
        out_specs=VMEM,
        scratch_shapes=[pltpu.SemaphoreType.DMA((2,))],
        compiler_params=pltpu.CompilerParams(vmem_limit_bytes=4 * MIB),
        cost_estimate=pl.CostEstimate(flops=10**8, transcendentals=0, bytes_accessed=10**6),
        name="front",
    )(stored)
    packed = pack(pack_kernel, 2, asked, near)
    packed += pack(relay_kernel, 1, asked, beside)
    chunks = []
    for block, source in zip(packed, (behind_of, ahead_of, relay_of)):
        chunks.append(from_sources(block, source).reshape(CAP * TILE, model_width))
    queries, tops, totals, mixed = pl.pallas_call(
        own_kernel,
        out_shape=[query, stat, stat, mix],
        in_specs=[SMEM, SMEM] + [VMEM] * 5,
        out_specs=[VMEM] * 4,
        scratch_shapes=[
            pltpu.VMEM((CAP * TILE, model_width), bf16),
            pltpu.VMEM((CAP * TILE, model_width), bf16),
            pltpu.VMEM((CAP, model_width, TILE), bf16),
            pltpu.SMEM((2 * own + 1,), jnp.int32),
        ],
        compiler_params=pltpu.CompilerParams(vmem_limit_bytes=12 * MIB),
        cost_estimate=pl.CostEstimate(flops=6 * 10**9, transcendentals=0, bytes_accessed=10**7),
        name="own",
    )(
        neighbour_tiles,
        neighbour_live,
        near.reshape(own * TILE, model_width),
        beside.reshape(own * TILE, model_width),
        w_keyval,
        mesh_latents,
        w_query,
    )

    for stage in STAGES:
        tops, totals, mixed = pl.pallas_call(
            functools.partial(chunk_kernel, SOURCES[stage], own),
            out_shape=[stat, stat, mix],
            in_specs=[SMEM, SMEM] + [VMEM] * 6,
            out_specs=[VMEM] * 3,
            scratch_shapes=[
                pltpu.VMEM((CAP * TILE, model_width), bf16),
                pltpu.VMEM((CAP, model_width, TILE), bf16),
            ],
            input_output_aliases={4: 0, 5: 1, 6: 2},
            compiler_params=pltpu.CompilerParams(vmem_limit_bytes=12 * MIB),
            cost_estimate=pl.CostEstimate(flops=2 * 10**9, transcendentals=0, bytes_accessed=10**6),
            name="chunk",
        )(neighbour_tiles, neighbour_live, w_keyval, queries, tops, totals, mixed, chunks[stage])
    return pl.pallas_call(
        functools.partial(last_kernel, SOURCES[LAST], own),
        out_shape=jax.ShapeDtypeStruct(mesh_latents.shape, f32),
        in_specs=[SMEM, SMEM] + [VMEM] * 8,
        out_specs=VMEM,
        scratch_shapes=[pltpu.VMEM(shape.shape, f32) for shape in (stat, stat, mix)]
        + [
            pltpu.VMEM((CAP * TILE, model_width), bf16),
            pltpu.VMEM((CAP, model_width, TILE), bf16),
        ],
        compiler_params=pltpu.CompilerParams(vmem_limit_bytes=12 * MIB),
        cost_estimate=pl.CostEstimate(flops=3 * 10**9, transcendentals=0, bytes_accessed=10**6),
        name="last",
    )(neighbour_tiles, neighbour_live, w_keyval, queries, tops, totals, mixed, chunks[LAST], mesh_latents, w_out)


def solution(mesh):
    return jax.shard_map(
        per_device,
        mesh=mesh,
        in_specs=(
            P(("groups", "nodes"), None),
            P(("groups", "nodes"), None),
            P("nodes", None),
            P("nodes", None),
            P(),
            P(),
            P(),
        ),
        out_specs=P(("groups", "nodes"), None),
        check_vma=False,
    )
```

```python
import functools

import jax
import jax.numpy as jnp
from jax import lax
from jax.experimental import pallas as pl
from jax.experimental.pallas import tpu as pltpu
from jax.sharding import PartitionSpec as P


HEADS = 16
TILE = 128
REACH = 2
CAP = 2
LOW = -1e30

SMEM = pl.BlockSpec(memory_space=pltpu.SMEM)
VMEM = pl.BlockSpec(memory_space=pltpu.VMEM)
HBM = pl.BlockSpec(memory_space=pltpu.HBM)
MIB = 1 << 20


def partner_of(i, n):
    return i + 1 - 2 * (i % 2)


def cross_of(i, n):
    return (i + n - 1 + 2 * (i % 2)) % n


def relay_of(i, n):
    return (i + n - REACH + 2 * REACH * (i % 2)) % n


def ahead_of(i, n):
    return (i + REACH) % n


def behind_of(i, n):
    return (i + n - REACH) % n


SOURCES = (behind_of, ahead_of, cross_of)
STAGES = (0, 1)
LAST = 2


def span_of(listed, base, own):
    low = jnp.int32(own)
    high = jnp.int32(-1)
    for entry in listed:
        local = entry - base
        held = (local >= 0) & (local < own)
        low = jnp.minimum(low, jnp.where(held, local, own))
        high = jnp.maximum(high, jnp.where(held, local, -1))
    return low, high


def entries(ref):
    return [ref[i, j] for i in range(ref.shape[0]) for j in range(ref.shape[1])]


def copy_listed(listed, base, grid, out):
    own = grid.shape[0]
    low, high = span_of(listed, base, own)
    out[0] = grid[jnp.where(high < 0, 0, low)]
    out[1] = grid[jnp.maximum(high, 0)]


def pack_kernel(from_ahead, from_behind, grid, to_ahead, to_behind):
    base = lax.axis_index("nodes") * grid.shape[0]
    copy_listed(entries(from_ahead), base, grid, to_ahead)
    copy_listed(entries(from_behind), base, grid, to_behind)


def relay_kernel(from_ahead, from_behind, grid, out):
    me = lax.axis_index("nodes")
    base = partner_of(me, lax.axis_size("nodes")) * grid.shape[0]
    even = me % 2 == 0
    listed = [
        jnp.where(even, ahead, behind)
        for ahead, behind in zip(entries(from_ahead), entries(from_behind))
    ]
    copy_listed(listed, base, grid, out)


def pack(kernel, count, asked, grid):
    shape = jax.ShapeDtypeStruct((CAP,) + grid.shape[1:], grid.dtype)
    return pl.pallas_call(
        kernel,
        out_shape=[shape] * count,
        in_specs=[SMEM, SMEM, VMEM],
        out_specs=[VMEM] * count,
        compiler_params=pltpu.CompilerParams(vmem_limit_bytes=4 * MIB),
        cost_estimate=pl.CostEstimate(flops=2 * 10**9, transcendentals=0, bytes_accessed=10**6),
    )(*asked, grid)


def project(rows_ref, w_keyval, keys, values, model_width):
    rows = rows_ref.shape[0]
    step = 256
    depth = min(rows, 512)
    for at in range(0, rows, depth):
        block = rows_ref[at : at + depth, :]
        for column in range(0, model_width, step):
            part = jnp.dot(
                block, w_keyval[:, column : column + step], preferred_element_type=jnp.float32
            )
            keys[at : at + depth, column : column + step] = part.astype(jnp.bfloat16)
            part = jnp.dot(
                block,
                w_keyval[:, model_width + column : model_width + column + step],
                preferred_element_type=jnp.float32,
            )
            turned = part.astype(jnp.bfloat16).T
            for k in range(depth // TILE):
                values[at // TILE + k, column : column + step, :] = turned[
                    :, k * TILE : (k + 1) * TILE
                ]


def add_tile(tile, mesh_tile, keys, values, queries, tops, totals, mixed):
    pairs = queries.shape[1]
    width = queries.shape[2]
    head = width // 2
    start = pl.multiple_of(tile * TILE, TILE)
    for pair in range(pairs):
        lanes = slice(pair * width, (pair + 1) * width)
        scores = jnp.dot(
            keys[pl.ds(start, TILE), lanes],
            queries[mesh_tile, pair],
            preferred_element_type=jnp.float32,
        )
        old = tops[mesh_tile, pair : pair + 1, :]
        new = jnp.maximum(old, jnp.max(scores, axis=0, keepdims=True))
        shrink = jnp.exp(old - new)
        raised = jnp.exp(scores - new)
        tops[mesh_tile, pair : pair + 1, :] = new
        totals[mesh_tile, pair : pair + 1, :] = totals[
            mesh_tile, pair : pair + 1, :
        ] * shrink + jnp.sum(raised, axis=0, keepdims=True)
        weights = raised.astype(jnp.bfloat16)
        for k in range(2):
            rows = slice(pair * width + k * head, pair * width + (k + 1) * head)
            cols = slice(k * TILE, (k + 1) * TILE)
            part = jnp.dot(
                values[tile, rows, :], weights[:, cols], preferred_element_type=jnp.float32
            )
            mixed[mesh_tile, rows, :] = mixed[mesh_tile, rows, :] * shrink[:, cols] + part


def lists(tiles_ref, live_ref, mesh_tile, wanted):
    found = jnp.bool_(False)
    for j in range(tiles_ref.shape[1]):
        found = found | ((live_ref[mesh_tile, j] > 0) & (tiles_ref[mesh_tile, j] == wanted))
    return found


def add_listed(count, keep, tiles_ref, live_ref, *state):
    mesh_tiles = tiles_ref.shape[0]

    def body(i, carry):
        tile = i // mesh_tiles
        mesh_tile = i % mesh_tiles
        wanted, fresh = keep(tile)

        @pl.when(fresh & lists(tiles_ref, live_ref, mesh_tile, wanted))
        def _():
            add_tile(tile, mesh_tile, *state)

        return carry

    lax.fori_loop(0, count * mesh_tiles, body, 0)


def front_kernel(grid_hbm, grid, sems):
    half = grid.shape[0] // 2
    copies = [
        pltpu.make_async_copy(
            grid_hbm.at[pl.ds(k * half, half)], grid.at[pl.ds(k * half, half)], sems.at[k]
        )
        for k in range(2)
    ]
    for copy in copies:
        copy.start()
    for copy in copies:
        copy.wait()


def query_kernel(mesh, w_query, queries):
    model_width = w_query.shape[0]
    head = queries.shape[2] // 2
    step = 256
    queries[...] = jnp.zeros(queries.shape, queries.dtype)
    for column in range(0, model_width, step):
        part = jnp.dot(
            mesh[...], w_query[:, column : column + step], preferred_element_type=jnp.float32
        )
        turned = (part.astype(jnp.bfloat16) * jnp.bfloat16(head ** -0.5)).T
        for m in range(queries.shape[0]):
            for h in range(step // head):
                which = column // head + h
                k = which % 2
                queries[m, which // 2, k * head : (k + 1) * head, k * TILE : (k + 1) * TILE] = turned[
                    h * head : (h + 1) * head, m * TILE : (m + 1) * TILE
                ]


def own_kernel(tiles_ref, live_ref, grid, beside, w_keyval, queries, tops, totals, mixed, rows, keys, values, found):
    own = grid.shape[0] // TILE
    mesh_tiles = tiles_ref.shape[0]
    tops[...] = jnp.full(tops.shape, LOW, jnp.float32)
    totals[...] = jnp.zeros(totals.shape, jnp.float32)
    mixed[...] = jnp.zeros(mixed.shape, jnp.float32)
    me = lax.axis_index("nodes")
    base = me * own
    base_beside = partner_of(me, lax.axis_size("nodes")) * own
    masks = []
    for m in range(mesh_tiles):
        mask = jnp.int32(0)
        for j in range(tiles_ref.shape[1]):
            tile = tiles_ref[m, j]
            here = tile - base
            there = tile - base_beside
            bit = jnp.where((here >= 0) & (here < own), here, -1)
            bit = jnp.where((there >= 0) & (there < own), there + own, bit)
            taken = (live_ref[m, j] > 0) & (bit >= 0)
            mask = mask | jnp.where(taken, lax.shift_left(jnp.int32(1), jnp.maximum(bit, 0)), 0)
        masks.append(mask)
    union = functools.reduce(jnp.bitwise_or, masks)
    count = jnp.int32(0)
    for bit in range(2 * own):
        found[count] = jnp.int32(bit)
        count = count + ((union >> bit) & 1)
    found[count] = jnp.int32(0)
    group = rows.shape[0] // TILE

    def body(g, carry):
        for k in range(group):
            bit = found[g * group + k]
            place = slice(k * TILE, (k + 1) * TILE)

            @pl.when(bit < own)
            def _():
                rows[place, :] = grid[pl.ds(pl.multiple_of(bit * TILE, TILE), TILE), :]

            @pl.when(bit >= own)
            def _():
                rows[place, :] = beside[pl.ds(pl.multiple_of((bit - own) * TILE, TILE), TILE), :]

        project(rows, w_keyval, keys, values, w_keyval.shape[0])

        def visit(i, inner):
            k = i // mesh_tiles
            m = i % mesh_tiles
            place = g * group + k
            mask = masks[0]
            for other in range(1, mesh_tiles):
                mask = jnp.where(m == other, masks[other], mask)
            taken = (lax.shift_right_logical(mask, found[place]) & 1) > 0

            @pl.when(taken & (place < count))
            def _():
                add_tile(k, m, keys, values, queries, tops, totals, mixed)

            return inner

        return lax.fori_loop(0, group * mesh_tiles, visit, carry)

    lax.fori_loop(0, (count + group - 1) // group, body, 0)


def chunk_update(source, own, tiles_ref, live_ref, rows, w_keyval, keys, values, queries, before, after):
    def carry_state():
        for old, new in zip(before, after):
            new[...] = old[...]

    me = lax.axis_index("nodes")
    n = lax.axis_size("nodes")
    listed = [
        jnp.where(live > 0, tile, -1)
        for tile, live in zip(entries(tiles_ref), entries(live_ref))
    ]
    base = source(me, n) * own
    low, high = span_of(listed, base, own)
    wanted = (base + low, jnp.where(low < high, base + high, -1))

    def keep(tile):
        found = jnp.where(tile == 0, wanted[0], wanted[1])
        return found, found >= 0

    @pl.when(high >= 0)
    def _():
        project(rows, w_keyval, keys, values, w_keyval.shape[0])
        carry_state()
        add_listed(CAP, keep, tiles_ref, live_ref, keys, values, queries, *after)

    @pl.when(high < 0)
    def _():
        carry_state()


def chunk_kernel(source, own, tiles_ref, live_ref, w_keyval, queries, tops_in, totals_in, mixed_in, chunk, tops, totals, mixed, keys, values):
    chunk_update(source, own, tiles_ref, live_ref, chunk, w_keyval, keys, values, queries, (tops_in, totals_in, mixed_in), (tops, totals, mixed))


def last_kernel(source, own, tiles_ref, live_ref, w_keyval, queries, tops_in, totals_in, mixed_in, chunk, mesh, w_out, out, tops, totals, mixed, keys, values):
    chunk_update(source, own, tiles_ref, live_ref, chunk, w_keyval, keys, values, queries, (tops_in, totals_in, mixed_in), (tops, totals, mixed))
    pairs = queries.shape[1]
    width = queries.shape[2]
    head = width // 2
    for m in range(queries.shape[0]):
        parts = []
        for pair in range(pairs):
            share = 1.0 / totals[m, pair : pair + 1, :]
            for k in range(2):
                rows = slice(pair * width + k * head, pair * width + (k + 1) * head)
                parts.append(
                    (mixed[m, rows, :] * share[:, k * TILE : (k + 1) * TILE]).astype(jnp.bfloat16)
                )
        attended = jnp.concatenate(parts, axis=0).T
        rows = slice(m * TILE, (m + 1) * TILE)
        out[rows, :] = mesh[rows, :].astype(jnp.float32) + jnp.dot(
            attended, w_out[...], preferred_element_type=jnp.float32
        )


def per_device(
    grid_latents, mesh_latents, neighbour_tiles, neighbour_live, w_query, w_keyval, w_out
):
    model_width = w_query.shape[0]
    own = grid_latents.shape[0] // TILE
    mesh_tiles = mesh_latents.shape[0] // TILE
    n = lax.axis_size("nodes")
    pairs = HEADS // 2
    width = model_width // pairs

    def to_sources(block, source):
        return lax.ppermute(block, "nodes", [(i, source(i, n)) for i in range(n)])

    def from_sources(block, source):
        return lax.ppermute(block, "nodes", [(source(i, n), i) for i in range(n)])

    f32 = jnp.float32
    bf16 = jnp.bfloat16
    stat = jax.ShapeDtypeStruct((mesh_tiles, pairs, 2 * TILE), f32)
    mix = jax.ShapeDtypeStruct((mesh_tiles, model_width, TILE), f32)
    query = jax.ShapeDtypeStruct((mesh_tiles, pairs, width, 2 * TILE), bf16)

    wanted = jnp.where(neighbour_live > 0, neighbour_tiles, -1)
    asked = []
    for source in (behind_of, ahead_of):
        asked.append(to_sources(wanted, source))
    tiled = grid_latents.reshape(own, TILE, model_width)
    beside = from_sources(tiled, partner_of)
    stored = pltpu.with_memory_space_constraint(tiled, pltpu.HBM)
    near = pl.pallas_call(
        front_kernel,
        out_shape=jax.ShapeDtypeStruct(tiled.shape, bf16),
        in_specs=[HBM],
        out_specs=VMEM,
        scratch_shapes=[pltpu.SemaphoreType.DMA((2,))],
        compiler_params=pltpu.CompilerParams(vmem_limit_bytes=4 * MIB),
        cost_estimate=pl.CostEstimate(flops=2 * 10**9, transcendentals=0, bytes_accessed=10**6),
        name="front",
    )(stored)
    queries = pl.pallas_call(
        query_kernel,
        out_shape=query,
        in_specs=[VMEM] * 2,
        out_specs=VMEM,
        compiler_params=pltpu.CompilerParams(vmem_limit_bytes=8 * MIB),
        cost_estimate=pl.CostEstimate(flops=10**9, transcendentals=0, bytes_accessed=10**6),
        name="query",
    )(mesh_latents, w_query)
    packed = pack(pack_kernel, 2, asked, near)
    packed += pack(relay_kernel, 1, asked, beside)
    chunks = []
    for block, source in zip(packed, (behind_of, ahead_of, relay_of)):
        chunks.append(from_sources(block, source).reshape(CAP * TILE, model_width))
    tops, totals, mixed = pl.pallas_call(
        own_kernel,
        out_shape=[stat, stat, mix],
        in_specs=[SMEM, SMEM] + [VMEM] * 4,
        out_specs=[VMEM] * 3,
        scratch_shapes=[
            pltpu.VMEM((CAP * TILE, model_width), bf16),
            pltpu.VMEM((CAP * TILE, model_width), bf16),
            pltpu.VMEM((CAP, model_width, TILE), bf16),
            pltpu.SMEM((2 * own + 1,), jnp.int32),
        ],
        compiler_params=pltpu.CompilerParams(vmem_limit_bytes=12 * MIB),
        cost_estimate=pl.CostEstimate(flops=6 * 10**9, transcendentals=0, bytes_accessed=10**7),
        name="own",
    )(
        neighbour_tiles,
        neighbour_live,
        near.reshape(own * TILE, model_width),
        beside.reshape(own * TILE, model_width),
        w_keyval,
        queries,
    )

    for stage in STAGES:
        tops, totals, mixed = pl.pallas_call(
            functools.partial(chunk_kernel, SOURCES[stage], own),
            out_shape=[stat, stat, mix],
            in_specs=[SMEM, SMEM] + [VMEM] * 6,
            out_specs=[VMEM] * 3,
            scratch_shapes=[
                pltpu.VMEM((CAP * TILE, model_width), bf16),
                pltpu.VMEM((CAP, model_width, TILE), bf16),
            ],
            input_output_aliases={4: 0, 5: 1, 6: 2},
            compiler_params=pltpu.CompilerParams(vmem_limit_bytes=12 * MIB),
            cost_estimate=pl.CostEstimate(flops=2 * 10**9, transcendentals=0, bytes_accessed=10**6),
            name="chunk",
        )(neighbour_tiles, neighbour_live, w_keyval, queries, tops, totals, mixed, chunks[stage])
    return pl.pallas_call(
        functools.partial(last_kernel, SOURCES[LAST], own),
        out_shape=jax.ShapeDtypeStruct(mesh_latents.shape, f32),
        in_specs=[SMEM, SMEM] + [VMEM] * 8,
        out_specs=VMEM,
        scratch_shapes=[pltpu.VMEM(shape.shape, f32) for shape in (stat, stat, mix)]
        + [
            pltpu.VMEM((CAP * TILE, model_width), bf16),
            pltpu.VMEM((CAP, model_width, TILE), bf16),
        ],
        compiler_params=pltpu.CompilerParams(vmem_limit_bytes=12 * MIB),
        cost_estimate=pl.CostEstimate(flops=3 * 10**9, transcendentals=0, bytes_accessed=10**6),
        name="last",
    )(neighbour_tiles, neighbour_live, w_keyval, queries, tops, totals, mixed, chunks[LAST], mesh_latents, w_out)


def solution(mesh):
    return jax.shard_map(
        per_device,
        mesh=mesh,
        in_specs=(
            P(("groups", "nodes"), None),
            P(("groups", "nodes"), None),
            P("nodes", None),
            P("nodes", None),
            P(),
            P(),
            P(),
        ),
        out_specs=P(("groups", "nodes"), None),
        check_vma=False,
    )
```

```python
import functools

import jax
import jax.numpy as jnp
from jax import lax
from jax.experimental import pallas as pl
from jax.experimental.pallas import tpu as pltpu
from jax.sharding import PartitionSpec as P


HEADS = 16
TILE = 128
REACH = 2
CAP = 2
LOW = -1e30

SMEM = pl.BlockSpec(memory_space=pltpu.SMEM)
VMEM = pl.BlockSpec(memory_space=pltpu.VMEM)
HBM = pl.BlockSpec(memory_space=pltpu.HBM)
MIB = 1 << 20


def partner_of(i, n):
    return i + 1 - 2 * (i % 2)


def cross_of(i, n):
    return (i + n - 1 + 2 * (i % 2)) % n


def relay_of(i, n):
    return (i + n - REACH + 2 * REACH * (i % 2)) % n


def ahead_of(i, n):
    return (i + REACH) % n


def behind_of(i, n):
    return (i + n - REACH) % n


SOURCES = (behind_of, ahead_of, cross_of)
STAGES = (0, 1)
LAST = 2


def span_of(listed, base, own):
    low = jnp.int32(own)
    high = jnp.int32(-1)
    for entry in listed:
        local = entry - base
        held = (local >= 0) & (local < own)
        low = jnp.minimum(low, jnp.where(held, local, own))
        high = jnp.maximum(high, jnp.where(held, local, -1))
    return low, high


def entries(ref):
    return [ref[i, j] for i in range(ref.shape[0]) for j in range(ref.shape[1])]


def copy_listed(listed, base, grid, out):
    own = grid.shape[0]
    low, high = span_of(listed, base, own)
    out[0] = grid[jnp.where(high < 0, 0, low)]
    out[1] = grid[jnp.maximum(high, 0)]


def pack_kernel(from_ahead, from_behind, grid, to_ahead, to_behind):
    base = lax.axis_index("nodes") * grid.shape[0]
    copy_listed(entries(from_ahead), base, grid, to_ahead)
    copy_listed(entries(from_behind), base, grid, to_behind)


def relay_kernel(from_ahead, from_behind, grid, out):
    me = lax.axis_index("nodes")
    base = partner_of(me, lax.axis_size("nodes")) * grid.shape[0]
    even = me % 2 == 0
    listed = [
        jnp.where(even, ahead, behind)
        for ahead, behind in zip(entries(from_ahead), entries(from_behind))
    ]
    copy_listed(listed, base, grid, out)


def pack(kernel, count, asked, grid):
    shape = jax.ShapeDtypeStruct((CAP,) + grid.shape[1:], grid.dtype)
    return pl.pallas_call(
        kernel,
        out_shape=[shape] * count,
        in_specs=[SMEM, SMEM, VMEM],
        out_specs=[VMEM] * count,
        compiler_params=pltpu.CompilerParams(vmem_limit_bytes=4 * MIB),
        cost_estimate=pl.CostEstimate(flops=2 * 10**9, transcendentals=0, bytes_accessed=10**6),
    )(*asked, grid)


def project(rows_ref, w_keyval, keys, values, model_width):
    rows = rows_ref.shape[0]
    step = 256
    depth = min(rows, 512)
    for at in range(0, rows, depth):
        block = rows_ref[at : at + depth, :]
        for column in range(0, model_width, step):
            part = jnp.dot(
                block, w_keyval[:, column : column + step], preferred_element_type=jnp.float32
            )
            keys[at : at + depth, column : column + step] = part.astype(jnp.bfloat16)
            part = jnp.dot(
                block,
                w_keyval[:, model_width + column : model_width + column + step],
                preferred_element_type=jnp.float32,
            )
            turned = part.astype(jnp.bfloat16).T
            for k in range(depth // TILE):
                values[at // TILE + k, column : column + step, :] = turned[
                    :, k * TILE : (k + 1) * TILE
                ]


def add_tiles(tiles, mesh_tile, keys, values, queries, tops, totals, mixed):
    pairs = queries.shape[1]
    width = queries.shape[2]
    head = width // 2
    starts = [pl.multiple_of(tile * TILE, TILE) for tile in tiles]
    for pair in range(pairs):
        lanes = slice(pair * width, (pair + 1) * width)
        scores = [
            jnp.dot(
                keys[pl.ds(start, TILE), lanes],
                queries[mesh_tile, pair],
                preferred_element_type=jnp.float32,
            )
            for start in starts
        ]
        old = tops[mesh_tile, pair : pair + 1, :]
        highest = functools.reduce(jnp.maximum, scores)
        new = jnp.maximum(old, jnp.max(highest, axis=0, keepdims=True))
        shrink = jnp.exp(old - new)
        raised = [jnp.exp(part - new) for part in scores]
        tops[mesh_tile, pair : pair + 1, :] = new
        totals[mesh_tile, pair : pair + 1, :] = totals[
            mesh_tile, pair : pair + 1, :
        ] * shrink + jnp.sum(functools.reduce(jnp.add, raised), axis=0, keepdims=True)
        weights = jnp.concatenate([part.astype(jnp.bfloat16) for part in raised], axis=0)
        for k in range(2):
            rows = slice(pair * width + k * head, pair * width + (k + 1) * head)
            cols = slice(k * TILE, (k + 1) * TILE)
            part = jnp.dot(
                jnp.concatenate([values[tile, rows, :] for tile in tiles], axis=1),
                weights[:, cols],
                preferred_element_type=jnp.float32,
            )
            mixed[mesh_tile, rows, :] = mixed[mesh_tile, rows, :] * shrink[:, cols] + part


def add_pair(first, second, mesh_tile, *state):
    @pl.when(first & second)
    def _():
        add_tiles((0, 1), mesh_tile, *state)

    @pl.when(first != second)
    def _():
        add_tiles((jnp.where(first, 0, 1),), mesh_tile, *state)


def lists(tiles_ref, live_ref, mesh_tile, wanted):
    found = jnp.bool_(False)
    for j in range(tiles_ref.shape[1]):
        found = found | ((live_ref[mesh_tile, j] > 0) & (tiles_ref[mesh_tile, j] == wanted))
    return found


def add_listed(wanted, tiles_ref, live_ref, *state):
    def body(mesh_tile, carry):
        first, second = (
            (tile >= 0) & lists(tiles_ref, live_ref, mesh_tile, tile) for tile in wanted
        )
        add_pair(first, second, mesh_tile, *state)
        return carry

    lax.fori_loop(0, tiles_ref.shape[0], body, 0)


def front_kernel(grid_hbm, grid, sems):
    half = grid.shape[0] // 2
    copies = [
        pltpu.make_async_copy(
            grid_hbm.at[pl.ds(k * half, half)], grid.at[pl.ds(k * half, half)], sems.at[k]
        )
        for k in range(2)
    ]
    for copy in copies:
        copy.start()
    for copy in copies:
        copy.wait()


def query_kernel(mesh, w_query, queries):
    model_width = w_query.shape[0]
    head = queries.shape[2] // 2
    step = 256
    queries[...] = jnp.zeros(queries.shape, queries.dtype)
    for column in range(0, model_width, step):
        part = jnp.dot(
            mesh[...], w_query[:, column : column + step], preferred_element_type=jnp.float32
        )
        turned = (part.astype(jnp.bfloat16) * jnp.bfloat16(head ** -0.5)).T
        for m in range(queries.shape[0]):
            for h in range(step // head):
                which = column // head + h
                k = which % 2
                queries[m, which // 2, k * head : (k + 1) * head, k * TILE : (k + 1) * TILE] = turned[
                    h * head : (h + 1) * head, m * TILE : (m + 1) * TILE
                ]


def own_kernel(tiles_ref, live_ref, grid, beside, w_keyval, queries, tops, totals, mixed, rows, keys, values, found):
    own = grid.shape[0] // TILE
    mesh_tiles = tiles_ref.shape[0]
    tops[...] = jnp.full(tops.shape, LOW, jnp.float32)
    totals[...] = jnp.zeros(totals.shape, jnp.float32)
    mixed[...] = jnp.zeros(mixed.shape, jnp.float32)
    me = lax.axis_index("nodes")
    base = me * own
    base_beside = partner_of(me, lax.axis_size("nodes")) * own
    masks = []
    for m in range(mesh_tiles):
        mask = jnp.int32(0)
        for j in range(tiles_ref.shape[1]):
            tile = tiles_ref[m, j]
            here = tile - base
            there = tile - base_beside
            bit = jnp.where((here >= 0) & (here < own), here, -1)
            bit = jnp.where((there >= 0) & (there < own), there + own, bit)
            taken = (live_ref[m, j] > 0) & (bit >= 0)
            mask = mask | jnp.where(taken, lax.shift_left(jnp.int32(1), jnp.maximum(bit, 0)), 0)
        masks.append(mask)
    union = functools.reduce(jnp.bitwise_or, masks)
    shared = functools.reduce(jnp.bitwise_and, masks)
    leading = masks[0] & ~shared
    count = jnp.int32(0)
    for members in (leading, shared, union & ~shared & ~leading):
        for bit in range(2 * own):
            found[count] = jnp.int32(bit)
            count = count + ((members >> bit) & 1)
    found[count] = jnp.int32(0)
    group = rows.shape[0] // TILE

    def body(g, carry):
        for k in range(group):
            bit = found[g * group + k]
            place = slice(k * TILE, (k + 1) * TILE)

            @pl.when(bit < own)
            def _():
                rows[place, :] = grid[pl.ds(pl.multiple_of(bit * TILE, TILE), TILE), :]

            @pl.when(bit >= own)
            def _():
                rows[place, :] = beside[pl.ds(pl.multiple_of((bit - own) * TILE, TILE), TILE), :]

        project(rows, w_keyval, keys, values, w_keyval.shape[0])

        def visit(m, inner):
            mask = masks[0]
            for other in range(1, mesh_tiles):
                mask = jnp.where(m == other, masks[other], mask)
            first, second = (
                ((lax.shift_right_logical(mask, found[place]) & 1) > 0) & (place < count)
                for place in (g * group, g * group + 1)
            )
            add_pair(first, second, m, keys, values, queries, tops, totals, mixed)
            return inner

        return lax.fori_loop(0, mesh_tiles, visit, carry)

    lax.fori_loop(0, (count + group - 1) // group, body, 0)


def chunk_update(source, own, tiles_ref, live_ref, rows, w_keyval, keys, values, queries, before, after):
    def carry_state():
        for old, new in zip(before, after):
            new[...] = old[...]

    me = lax.axis_index("nodes")
    n = lax.axis_size("nodes")
    listed = [
        jnp.where(live > 0, tile, -1)
        for tile, live in zip(entries(tiles_ref), entries(live_ref))
    ]
    base = source(me, n) * own
    low, high = span_of(listed, base, own)
    wanted = (base + low, jnp.where(low < high, base + high, -1))

    @pl.when(high >= 0)
    def _():
        project(rows, w_keyval, keys, values, w_keyval.shape[0])
        carry_state()
        add_listed(wanted, tiles_ref, live_ref, keys, values, queries, *after)

    @pl.when(high < 0)
    def _():
        carry_state()


def chunk_kernel(source, own, tiles_ref, live_ref, w_keyval, queries, tops_in, totals_in, mixed_in, chunk, tops, totals, mixed, keys, values):
    chunk_update(source, own, tiles_ref, live_ref, chunk, w_keyval, keys, values, queries, (tops_in, totals_in, mixed_in), (tops, totals, mixed))


def last_kernel(source, own, tiles_ref, live_ref, w_keyval, queries, tops_in, totals_in, mixed_in, chunk, mesh, w_out, out, tops, totals, mixed, keys, values):
    chunk_update(source, own, tiles_ref, live_ref, chunk, w_keyval, keys, values, queries, (tops_in, totals_in, mixed_in), (tops, totals, mixed))
    pairs = queries.shape[1]
    width = queries.shape[2]
    head = width // 2
    for m in range(queries.shape[0]):
        parts = []
        for pair in range(pairs):
            share = 1.0 / totals[m, pair : pair + 1, :]
            for k in range(2):
                rows = slice(pair * width + k * head, pair * width + (k + 1) * head)
                parts.append(
                    (mixed[m, rows, :] * share[:, k * TILE : (k + 1) * TILE]).astype(jnp.bfloat16)
                )
        attended = jnp.concatenate(parts, axis=0).T
        rows = slice(m * TILE, (m + 1) * TILE)
        out[rows, :] = mesh[rows, :].astype(jnp.float32) + jnp.dot(
            attended, w_out[...], preferred_element_type=jnp.float32
        )


def per_device(
    grid_latents, mesh_latents, neighbour_tiles, neighbour_live, w_query, w_keyval, w_out
):
    model_width = w_query.shape[0]
    own = grid_latents.shape[0] // TILE
    mesh_tiles = mesh_latents.shape[0] // TILE
    n = lax.axis_size("nodes")
    pairs = HEADS // 2
    width = model_width // pairs

    def to_sources(block, source):
        return lax.ppermute(block, "nodes", [(i, source(i, n)) for i in range(n)])

    def from_sources(block, source):
        return lax.ppermute(block, "nodes", [(source(i, n), i) for i in range(n)])

    f32 = jnp.float32
    bf16 = jnp.bfloat16
    stat = jax.ShapeDtypeStruct((mesh_tiles, pairs, 2 * TILE), f32)
    mix = jax.ShapeDtypeStruct((mesh_tiles, model_width, TILE), f32)
    query = jax.ShapeDtypeStruct((mesh_tiles, pairs, width, 2 * TILE), bf16)

    wanted = jnp.where(neighbour_live > 0, neighbour_tiles, -1)
    asked = []
    for source in (behind_of, ahead_of):
        asked.append(to_sources(wanted, source))
    tiled = grid_latents.reshape(own, TILE, model_width)
    beside = from_sources(tiled, partner_of)
    stored = pltpu.with_memory_space_constraint(tiled, pltpu.HBM)
    near = pl.pallas_call(
        front_kernel,
        out_shape=jax.ShapeDtypeStruct(tiled.shape, bf16),
        in_specs=[HBM],
        out_specs=VMEM,
        scratch_shapes=[pltpu.SemaphoreType.DMA((2,))],
        compiler_params=pltpu.CompilerParams(vmem_limit_bytes=4 * MIB),
        cost_estimate=pl.CostEstimate(flops=10**8, transcendentals=0, bytes_accessed=10**6),
        name="front",
    )(stored)
    queries = pl.pallas_call(
        query_kernel,
        out_shape=query,
        in_specs=[VMEM] * 2,
        out_specs=VMEM,
        compiler_params=pltpu.CompilerParams(vmem_limit_bytes=8 * MIB),
        cost_estimate=pl.CostEstimate(flops=10**9, transcendentals=0, bytes_accessed=10**6),
        name="query",
    )(mesh_latents, w_query)
    packed = pack(pack_kernel, 2, asked, near)
    packed += pack(relay_kernel, 1, asked, beside)
    chunks = []
    for block, source in zip(packed, (behind_of, ahead_of, relay_of)):
        chunks.append(from_sources(block, source).reshape(CAP * TILE, model_width))
    tops, totals, mixed = pl.pallas_call(
        own_kernel,
        out_shape=[stat, stat, mix],
        in_specs=[SMEM, SMEM] + [VMEM] * 4,
        out_specs=[VMEM] * 3,
        scratch_shapes=[
            pltpu.VMEM((CAP * TILE, model_width), bf16),
            pltpu.VMEM((CAP * TILE, model_width), bf16),
            pltpu.VMEM((CAP, model_width, TILE), bf16),
            pltpu.SMEM((2 * own + 2,), jnp.int32),
        ],
        compiler_params=pltpu.CompilerParams(vmem_limit_bytes=12 * MIB),
        cost_estimate=pl.CostEstimate(flops=6 * 10**9, transcendentals=0, bytes_accessed=10**7),
        name="own",
    )(
        neighbour_tiles,
        neighbour_live,
        near.reshape(own * TILE, model_width),
        beside.reshape(own * TILE, model_width),
        w_keyval,
        queries,
    )

    for stage in STAGES:
        tops, totals, mixed = pl.pallas_call(
            functools.partial(chunk_kernel, SOURCES[stage], own),
            out_shape=[stat, stat, mix],
            in_specs=[SMEM, SMEM] + [VMEM] * 6,
            out_specs=[VMEM] * 3,
            scratch_shapes=[
                pltpu.VMEM((CAP * TILE, model_width), bf16),
                pltpu.VMEM((CAP, model_width, TILE), bf16),
            ],
            input_output_aliases={4: 0, 5: 1, 6: 2},
            compiler_params=pltpu.CompilerParams(vmem_limit_bytes=12 * MIB),
            cost_estimate=pl.CostEstimate(flops=2 * 10**9, transcendentals=0, bytes_accessed=10**6),
            name="chunk",
        )(neighbour_tiles, neighbour_live, w_keyval, queries, tops, totals, mixed, chunks[stage])
    return pl.pallas_call(
        functools.partial(last_kernel, SOURCES[LAST], own),
        out_shape=jax.ShapeDtypeStruct(mesh_latents.shape, f32),
        in_specs=[SMEM, SMEM] + [VMEM] * 8,
        out_specs=VMEM,
        scratch_shapes=[pltpu.VMEM(shape.shape, f32) for shape in (stat, stat, mix)]
        + [
            pltpu.VMEM((CAP * TILE, model_width), bf16),
            pltpu.VMEM((CAP, model_width, TILE), bf16),
        ],
        compiler_params=pltpu.CompilerParams(vmem_limit_bytes=12 * MIB),
        cost_estimate=pl.CostEstimate(flops=3 * 10**9, transcendentals=0, bytes_accessed=10**6),
        name="last",
    )(neighbour_tiles, neighbour_live, w_keyval, queries, tops, totals, mixed, chunks[LAST], mesh_latents, w_out)


def solution(mesh):
    return jax.shard_map(
        per_device,
        mesh=mesh,
        in_specs=(
            P(("groups", "nodes"), None),
            P(("groups", "nodes"), None),
            P("nodes", None),
            P("nodes", None),
            P(),
            P(),
            P(),
        ),
        out_specs=P(("groups", "nodes"), None),
        check_vma=False,
    )
```
